16 devices in a mesh: req: 2 (over y, z), cp: 8 (over x, core).
Axes of the slice: x: 4, y: 2, z: 1, core: 2. Of those that a mesh axis runs over, the one named last changes fastest.
The devices are a block of a 4x4x8 slice.
Arguments:
- hidden: bfloat16 [1024, 1536], P(('req', 'cp')), parts along dimension 0
- prefix_k: bfloat16 [4, 16384, 256], P(None, 'req', 'cp'), parts along dimension 1
- prefix_v: bfloat16 [4, 16384, 256], P(None, 'req', 'cp'), parts along dimension 1
- gain_attn: bfloat16 [4, 1536], replicated
- gain_mlp: bfloat16 [4, 1536], replicated
- w_query: bfloat16 [4, 1536, 12, 128], replicated
- w_key: bfloat16 [4, 1536, 2, 128], replicated
- w_value: bfloat16 [4, 1536, 2, 128], replicated
- w_out: bfloat16 [4, 12, 128, 1536], replicated
- w_gate: bfloat16 [4, 1536, 8960], replicated
- w_up: bfloat16 [4, 1536, 8960], replicated
- w_down: bfloat16 [4, 8960, 1536], replicated
Outputs:
- output 1: bfloat16 [1024, 1536], P(('req', 'cp')), parts along dimension 0
- output 2: bfloat16 [4, 17408, 256], P(None, 'req', 'cp'), parts along dimension 1
- output 3: bfloat16 [4, 17408, 256], P(None, 'req', 'cp'), parts along dimension 1
There are 2 independent parts. The reference program is written for one: setup_inputs(seed, part) draws one part's arguments, and reference() takes and returns one part's arrays. A program takes and returns all parts, laid end to end along the dimension named above; an argument that names none is the same for every part.
All inputs are finite; a program needn't handle non-finite values.
Results may differ from the reference program's by a relative error of at most 0.02.
Values are sent between devices in bfloat16 or wider.
A program may use at most 768 MiB of HBM per device.

```python
import math
import jax
import jax.numpy as jnp
from jax import lax

D = 1536
HEADS = 12
KV_HEADS = 2
HEAD = 128
FF = 8960
LAYERS = 4
CP_SIZE = 8
TOK_DEV = 64
PREFIX_DEV = 1024

SEQ_LEN = CP_SIZE * TOK_DEV
PREFIX = CP_SIZE * PREFIX_DEV
TOTAL = PREFIX + SEQ_LEN
KV_DIM = KV_HEADS * HEAD
GROUP_SIZE = HEADS // KV_HEADS
HALF_PIECE = TOK_DEV // 2
NORM_EPS = 1e-5
ROPE_THETA = 500000.0
SCORE_STD = math.sqrt(math.log(TOTAL / 8.0))


def normal_weight(key, shape, scale):
    return (jax.random.normal(key, shape, jnp.float32) * scale).astype(jnp.bfloat16)


def setup_inputs(seed: int = 0, part: int = 0) -> dict:
    shared_key = jax.random.key(seed)
    part_keys = jax.random.split(jax.random.fold_in(shared_key, part), 3)
    layer_keys = jax.random.split(shared_key, 9)
    qk_scale = math.sqrt(SCORE_STD)
    out_scale = 2.0 / math.sqrt(LAYERS)
    gain_attn = 1.0 + 0.25 * jax.random.normal(layer_keys[0], (LAYERS, D), jnp.float32)
    gain_mlp = 1.0 + 0.25 * jax.random.normal(layer_keys[1], (LAYERS, D), jnp.float32)
    return {
        'hidden': normal_weight(part_keys[0], (SEQ_LEN, D), 1.0),
        'prefix_k': normal_weight(part_keys[1], (LAYERS, PREFIX, KV_DIM), qk_scale),
        'prefix_v': normal_weight(part_keys[2], (LAYERS, PREFIX, KV_DIM), 1.0),
        'gain_attn': gain_attn.astype(jnp.bfloat16),
        'gain_mlp': gain_mlp.astype(jnp.bfloat16),
        'w_query': normal_weight(layer_keys[2], (LAYERS, D, HEADS, HEAD), qk_scale / math.sqrt(D)),
        'w_key': normal_weight(layer_keys[3], (LAYERS, D, KV_HEADS, HEAD), qk_scale / math.sqrt(D)),
        'w_value': normal_weight(layer_keys[4], (LAYERS, D, KV_HEADS, HEAD), 1.0 / math.sqrt(D)),
        'w_out': normal_weight(layer_keys[5], (LAYERS, HEADS, HEAD, D), out_scale / math.sqrt(HEADS * HEAD)),
        'w_gate': normal_weight(layer_keys[6], (LAYERS, D, FF), 1.0 / math.sqrt(D)),
        'w_up': normal_weight(layer_keys[7], (LAYERS, D, FF), 1.0 / math.sqrt(D)),
        'w_down': normal_weight(layer_keys[8], (LAYERS, FF, D), out_scale / math.sqrt(FF)),
    }


def rms_norm(hidden, gain):
    hidden_f32 = hidden.astype(jnp.float32)
    inv_rms = lax.rsqrt(jnp.mean(hidden_f32 * hidden_f32, axis=-1, keepdims=True) + NORM_EPS)
    return (hidden_f32 * inv_rms * gain.astype(jnp.float32)).astype(jnp.bfloat16)


def rope_tables(positions):
    inv_freq = ROPE_THETA ** (-jnp.arange(0, HEAD, 2, dtype=jnp.float32) / HEAD)
    angles = positions.astype(jnp.float32)[:, None] * inv_freq[None, :]
    return jnp.cos(angles), jnp.sin(angles)


def rope_rotate(projected, cos_tab, sin_tab):
    half_dim = projected.shape[-1] // 2
    lower_half = projected[..., :half_dim]
    upper_half = projected[..., half_dim:]
    cos_part = cos_tab[:, None, :]
    sin_part = sin_tab[:, None, :]
    return jnp.concatenate([lower_half * cos_part - upper_half * sin_part, upper_half * cos_part + lower_half * sin_part], axis=-1)


def stored_to_natural(row_data):
    num_cols = row_data.shape[-1]
    blocks = row_data.reshape(CP_SIZE, 2, HALF_PIECE, num_cols)
    return jnp.concatenate([blocks[:, 0], jnp.flip(blocks[:, 1], axis=0)], axis=0).reshape(SEQ_LEN, num_cols)


def natural_to_stored(row_data):
    num_cols = row_data.shape[-1]
    pieces = row_data.reshape(2, CP_SIZE, HALF_PIECE, num_cols)
    return jnp.stack([pieces[0], jnp.flip(pieces[1], axis=0)], axis=1).reshape(SEQ_LEN, num_cols)


def attend_block(query_blk, query_pos, key_f32, value_f32):
    key_pos = jnp.arange(TOTAL)
    allowed = key_pos[None, :] <= query_pos[:, None]
    scores = jnp.einsum('tkgd,skd->kgts', query_blk.astype(jnp.float32), key_f32) * HEAD ** -0.5
    scores = jnp.where(allowed, scores, -jnp.inf)
    row_max = scores.max(axis=-1, keepdims=True)
    exp_scores = jnp.exp(scores - row_max)
    probabilities = (exp_scores / exp_scores.sum(axis=-1, keepdims=True)).astype(jnp.bfloat16)
    attn_out = jnp.einsum('kgts,skd->tkgd', probabilities.astype(jnp.float32), value_f32)
    return attn_out.astype(jnp.bfloat16)


def decoder_layer(hidden, layer_params):
    gain_attn, gain_mlp, w_query, w_key, w_value, w_out, w_gate, w_up, w_down, prefix_keys, prefix_vals = layer_params
    positions = PREFIX + jnp.arange(SEQ_LEN)
    cos_tab, sin_tab = rope_tables(positions)
    normed = rms_norm(hidden, gain_attn)
    queries = jnp.dot(normed, w_query.reshape(D, HEADS * HEAD), preferred_element_type=jnp.float32)
    queries = rope_rotate(queries.reshape(SEQ_LEN, HEADS, HEAD), cos_tab, sin_tab).astype(jnp.bfloat16)
    keys_new = jnp.dot(normed, w_key.reshape(D, KV_DIM), preferred_element_type=jnp.float32)
    keys_new = rope_rotate(keys_new.reshape(SEQ_LEN, KV_HEADS, HEAD), cos_tab, sin_tab).astype(jnp.bfloat16).reshape(SEQ_LEN, KV_DIM)
    values_new = jnp.dot(normed, w_value.reshape(D, KV_DIM), preferred_element_type=jnp.float32).astype(jnp.bfloat16)
    key_f32 = jnp.concatenate([prefix_keys, keys_new], axis=0).astype(jnp.float32).reshape(TOTAL, KV_HEADS, HEAD)
    value_f32 = jnp.concatenate([prefix_vals, values_new], axis=0).astype(jnp.float32).reshape(TOTAL, KV_HEADS, HEAD)
    query_blocks = queries.reshape(CP_SIZE, TOK_DEV, KV_HEADS, GROUP_SIZE, HEAD)
    pos_blocks = positions.reshape(CP_SIZE, TOK_DEV)
    attn_out = lax.map(lambda query_pair: attend_block(query_pair[0], query_pair[1], key_f32, value_f32), (query_blocks, pos_blocks))
    attn_out = attn_out.reshape(SEQ_LEN, HEADS * HEAD)
    hidden = (hidden.astype(jnp.float32) + jnp.dot(attn_out, w_out.reshape(HEADS * HEAD, D), preferred_element_type=jnp.float32)).astype(jnp.bfloat16)
    normed_mlp = rms_norm(hidden, gain_mlp)
    gate_proj = jnp.dot(normed_mlp, w_gate, preferred_element_type=jnp.float32)
    up_proj = jnp.dot(normed_mlp, w_up, preferred_element_type=jnp.float32)
    gated_act = (jax.nn.silu(gate_proj) * up_proj).astype(jnp.bfloat16)
    hidden = (hidden.astype(jnp.float32) + jnp.dot(gated_act, w_down, preferred_element_type=jnp.float32)).astype(jnp.bfloat16)
    return hidden, (keys_new, values_new)


def reference(hidden, prefix_k, prefix_v, gain_attn, gain_mlp, w_query, w_key, w_value, w_out, w_gate, w_up, w_down):
    natural = stored_to_natural(hidden)
    final_hidden, new_caches = lax.scan(decoder_layer, natural, (gain_attn, gain_mlp, w_query, w_key, w_value, w_out, w_gate, w_up, w_down, prefix_k, prefix_v))
    cache_k = jnp.concatenate([prefix_k, new_caches[0]], axis=1)
    cache_v = jnp.concatenate([prefix_v, new_caches[1]], axis=1)
    return natural_to_stored(final_hidden), cache_k, cache_v
```

```python
import functools
import math

import jax
import jax.numpy as jnp
from jax import lax
from jax.experimental import pallas as pl
from jax.experimental.pallas import tpu as pltpu
from jax.sharding import PartitionSpec as P

NORM_EPS = 1e-5
ROPE_THETA = 500000.0
MESH = pl.DeviceIdType.MESH
F32 = jnp.float32
BF16 = jnp.bfloat16

COMM_CHUNK = 2048
KEY_CHUNK = 1024
FF_CHUNK = 640
SLOTS = 4


def rms(x, gain):
    xf = x.astype(F32)
    inv = lax.rsqrt(jnp.mean(xf * xf, axis=-1, keepdims=True) + NORM_EPS)
    return (xf * inv * gain.astype(F32)).astype(BF16)


def mm(a, b):
    return jnp.dot(a, b, preferred_element_type=F32)


def mm_t(a, b):
    return lax.dot_general(a, b, (((1,), (1,)), ((), ())), preferred_element_type=F32)


def kernel(cfg, x_in, pk, pv, g1, g2, wq, wkv, wo, wg, wu, wd, cos_ref, sin_ref,
           x_out, k_out, v_out,
           kv, gu, w2, wq_v, wkv_v, wo_v, nkv, kvs, qs, qr, h2, acc, part, x_s, att_own, att_snd, att_rcv,
           m_s, l_s, o_s, tr,
           lsem, ss_sib, ss_nbr, ss_fwd, rs_sib, rs_nbr, rs_fwd, nk_s, nk_r, q_sem, o_sem, h_sem, p_sem,
           wq_sem, wkv_sem, wo_sem, gu_sem, w2_sem):
    n, L, D, heads, kvh, hd, tok, cols, plen = cfg
    grp = heads // kvh
    per = n // kvh
    grows = grp * tok
    gcols = grp * hd
    nch = plen // COMM_CHUNK
    ff_half = wg.shape[2] // 2
    nff = ff_half // FF_CHUNK
    total_ff = L * nff
    scale = hd ** -0.5 * math.log2(math.e)

    me = lax.axis_index('cp')
    core = lax.rem(me, 2)
    chip = lax.div(me, 2)
    kvj = lax.div(me, per)
    quarter = lax.rem(me, per)
    sib = me + 1 - 2 * core
    nbr = kvj * per + lax.rem(quarter + 2, per)
    mate = 2 * (n // 2 - 1 - chip) + core

    def rows_of(dev):
        return pl.ds(pl.multiple_of(lax.rem(dev, per) * cols, cols), cols)

    my_rows = rows_of(me)
    nbr_rows = rows_of(nbr)
    sib_rows = rows_of(sib)
    sibnbr = kvj * per + lax.rem(lax.rem(sib, per) + 2, per)
    sibnbr_rows = rows_of(sibnbr)

    def rcopy(src, dst, s, r, dev):
        return pltpu.make_async_remote_copy(src_ref=src, dst_ref=dst, send_sem=s, recv_sem=r,
                                            device_id={'cp': dev}, device_id_type=MESH)

    def cpos(ch):
        return pl.ds(ch * COMM_CHUNK if isinstance(ch, int) else pl.multiple_of(ch * COMM_CHUNK, COMM_CHUNK), COMM_CHUNK)

    def wq_start(l):
        for h in range(heads):
            pltpu.make_async_copy(wq.at[l, h], wq_v.at[:, pl.ds(h * hd, hd)], wq_sem).start()
        pltpu.make_async_copy(wkv.at[l], wkv_v, wkv_sem).start()

    def wo_start(l):
        pltpu.make_async_copy(wo.at[l], wo_v, wo_sem).start()

    def ff_copies(g):
        l = lax.div(g, nff)
        off = pl.multiple_of(core * ff_half + lax.rem(g, nff) * FF_CHUNK, 128)
        slot = lax.rem(g, SLOTS)
        return (pltpu.make_async_copy(wg.at[l, :, pl.ds(off, FF_CHUNK)], gu.at[slot, :, pl.ds(0, FF_CHUNK)], gu_sem.at[slot, 0]),
                pltpu.make_async_copy(wu.at[l, :, pl.ds(off, FF_CHUNK)], gu.at[slot, :, pl.ds(FF_CHUNK, FF_CHUNK)], gu_sem.at[slot, 1]),
                pltpu.make_async_copy(wd.at[l, pl.ds(off, FF_CHUNK), :], w2.at[slot], w2_sem.at[slot]))

    def ff_start(g):
        for c in ff_copies(g):
            c.start()

    def own_local(l):
        pltpu.make_async_copy(pk.at[l], kv.at[l, 0, my_rows, :], lsem.at[l]).start()
        pltpu.make_async_copy(pv.at[l], kv.at[l, 1, my_rows, :], lsem.at[l]).start()

    def own_send(l):
        def body(ch, _):
            for i, src in enumerate((pk, pv)):
                rcopy(src.at[l, :, cpos(ch)], kv.at[l, i, my_rows, cpos(ch)], ss_nbr.at[l], rs_nbr.at[l, ch], nbr).start()
                rcopy(src.at[l, :, cpos(ch)], kv.at[l, i, my_rows, cpos(ch)], ss_sib.at[l], rs_sib.at[l, ch], sib).start()
            return 0
        lax.fori_loop(0, nch, body, 0)

    def forward(l, ch):
        blk = kv.at[l, :, nbr_rows, cpos(ch)]
        rcopy(blk, blk, ss_nbr.at[l], rs_nbr.at[l, ch], nbr).wait_recv()
        rcopy(blk, blk, ss_fwd.at[l], rs_fwd.at[l, ch], sib).start()

    def chunk_ready(l, ch):
        @pl.when(ch + 1 < nch)
        def _():
            forward(l, ch + 1)
        blk = kv.at[l, :, sib_rows, cpos(ch)]
        rcopy(blk, blk, ss_sib.at[l], rs_sib.at[l, ch], sib).wait_recv()
        blk = kv.at[l, :, sibnbr_rows, cpos(ch)]
        rcopy(blk, blk, ss_fwd.at[l], rs_fwd.at[l, ch], sib).wait_recv()

    barrier = pltpu.get_barrier_semaphore()
    for off in range(1, n):
        pl.semaphore_signal(barrier, inc=1, device_id={'cp': lax.rem(me + off, n)}, device_id_type=MESH)

    wq_start(0)
    own_local(0)
    wo_start(0)
    x_s[...] = x_in[...]
    pl.semaphore_wait(barrier, n - 1)
    own_send(0)

    def prime(g, _):
        ff_start(g)
        return 0
    lax.fori_loop(0, SLOTS, prime, 0)

    def local_rest(l, _):
        own_local(l)
        return 0
    lax.fori_loop(1, L, local_rest, 0)

    def token_pos(t, dev):
        half = tok // 2
        return jnp.where(t < half, dev * half + t, (2 * n - 1 - dev) * half + t - half)

    def reset(st):
        m_s[st] = jnp.full((grows, hd), -jnp.inf, F32)
        l_s[st] = jnp.zeros((grows, hd), F32)
        o_s[st] = jnp.zeros((grows, hd), F32)

    def fold(st, s, pv_dot):
        width = s.shape[1]
        m_prev = m_s[st]
        m_new = jnp.maximum(m_prev, jnp.max(s, axis=1, keepdims=True))
        alpha = jnp.exp2((m_prev - m_new) * scale)
        p = jnp.exp2((s - jnp.concatenate([m_new] * (width // hd), axis=1)) * scale)
        lsum = p[:, :hd]
        for b in range(1, width // hd):
            lsum = lsum + p[:, b * hd:(b + 1) * hd]
        m_s[st] = m_new
        l_s[st] = alpha * l_s[st] + lsum
        o_s[st] = alpha * o_s[st] + pv_dot(p.astype(BF16))

    def attend_prefix(l, st, q_at, ch):
        for sub in range(COMM_CHUNK // KEY_CHUNK):
            pos = pl.ds(pl.multiple_of(ch * COMM_CHUNK + sub * KEY_CHUNK, KEY_CHUNK), KEY_CHUNK)
            s = mm(q_at(), kv[l, 0, :, pos])
            fold(st, s, lambda p: mm_t(p, kv[l, 1, :, pos]))

    def attend_new(l, st, q_at, dev):
        s = mm_t(q_at(), nkv[l, 0])
        width = n * tok
        tq = lax.broadcasted_iota(jnp.int32, (grows, width), 0) & (tok - 1)
        col = lax.broadcasted_iota(jnp.int32, (grows, width), 1)
        tk = col & (tok - 1)
        dk = col >> (tok.bit_length() - 1)
        allowed = token_pos(tk, dk) <= token_pos(tq, dev)
        s = jnp.where(allowed, s, -jnp.inf)
        fold(st, s, lambda p: mm(p, nkv[l, 1]))

    def finish(st, dst):
        o = (o_s[st] / jnp.sum(l_s[st], axis=1, keepdims=True)).astype(BF16)
        for h in range(grp):
            dst[:, h * hd:(h + 1) * hd] = o[h * tok:(h + 1) * tok, :]

    own_q = pl.ds(pl.multiple_of(kvj * grows, grows), grows)
    mate_q = pl.ds(pl.multiple_of((1 - kvj) * grows, grows), grows)
    own_tok = pl.ds(pl.multiple_of(core * tok, tok), tok)
    sib_tok = pl.ds(pl.multiple_of((1 - core) * tok, tok), tok)
    my_new = pl.ds(pl.multiple_of(me * tok, tok), tok)

    def layer(l, _):
        @pl.when(l > 0)
        def _():
            forward(l, 0)
        h = rms(x_s[...], g1[l])
        pltpu.make_async_copy(wo.at[l], wq_v, wq_sem).wait()
        cos_t = cos_ref[...]
        sin_t = sin_ref[...]

        def rope(z):
            return (z * cos_t + pltpu.roll(z, hd // 2, 1) * sin_t).astype(BF16)

        for pr in range(heads // 2):
            y = mm(h, wq_v[:, 2 * pr * hd:(2 * pr + 2) * hd])
            for s in range(2):
                hh = 2 * pr + s
                qs[hh * tok:(hh + 1) * tok, :] = rope(y[:, s * hd:(s + 1) * hd])
        q_copy = rcopy(qs.at[mate_q, :], qr, q_sem.at[0], q_sem.at[1], mate)
        q_copy.start()
        pltpu.make_async_copy(wkv.at[l], wkv_v, wkv_sem).wait()
        for i in range(2):
            y = mm(h, wkv_v[:, i * kvh * hd:(i + 1) * kvh * hd])
            for j in range(kvh):
                z = y[:, j * hd:(j + 1) * hd]
                kvs[j, i] = rope(z) if i == 0 else z.astype(BF16)

        @pl.when(l + 1 < L)
        def _():
            wq_start(l + 1)

        for i in range(2):
            nkv[l, i, my_new, :] = kvs[kvj, i]

        def nk_copy(off):
            dst = lax.rem(me + off, n)
            return rcopy(kvs.at[lax.div(dst, per)], nkv.at[l, :, my_new, :], nk_s.at[off], nk_r.at[l, me], dst)

        for off in range(1, n):
            nk_copy(off).start()

        @pl.when(l + 1 < L)
        def _():
            own_send(l + 1)

        @pl.when(l == 0)
        def _():
            forward(l, 0)
        full = kv.at[l, :, my_rows, :]
        pltpu.make_async_copy(full, full, lsem.at[l]).wait()

        reset(0)
        reset(1)

        def own_chunk(ch, _):
            attend_prefix(l, 0, lambda: qs[own_q, :], ch)
            return 0

        def first_half(ch, _):
            chunk_ready(l, ch)
            return own_chunk(ch, 0)
        lax.fori_loop(0, nch // 2, first_half, 0)
        q_copy.wait_recv()

        def mate_chunk(ch, _):
            @pl.when(ch >= nch // 2)
            def _():
                chunk_ready(l, ch)
            attend_prefix(l, 1, lambda: qr[...], ch)
            return 0
        lax.fori_loop(0, nch, mate_chunk, 0)
        for off in range(1, n):
            src = lax.rem(me + off, n)
            blk = nkv.at[l, :, pl.ds(pl.multiple_of(src * tok, tok), tok), :]
            rcopy(blk, blk, nk_s.at[off], nk_r.at[l, src], src).wait_recv()
        attend_new(l, 1, lambda: qr[...], mate)
        finish(1, att_snd)
        o_copy = rcopy(att_snd, att_rcv, o_sem.at[0], o_sem.at[1], mate)
        o_copy.start()
        lax.fori_loop(nch // 2, nch, own_chunk, 0)
        attend_new(l, 0, lambda: qs[own_q, :], me)
        finish(0, att_own)

        pltpu.make_async_copy(wo.at[l], wo_v, wo_sem).wait()
        y = mm(att_own[...], wo_v[pl.ds(pl.multiple_of(kvj * gcols, gcols), gcols), :])
        o_copy.wait_recv()
        y = y + mm(att_rcv[...], wo_v[pl.ds(pl.multiple_of((1 - kvj) * gcols, gcols), gcols), :])
        x1 = (x_s[...].astype(F32) + y).astype(BF16)
        x_s[...] = x1
        h2[own_tok, :] = rms(x1, g2[l])
        h_copy = rcopy(h2.at[own_tok, :], h2.at[own_tok, :], h_sem.at[0], h_sem.at[1], sib)
        h_copy.start()

        @pl.when(l + 1 < L)
        def _():
            wo_start(l + 1)
        q_copy.wait_send()
        o_copy.wait_send()
        for off in range(1, n):
            nk_copy(off).wait_send()
        half = tok // 2
        for i, out in enumerate((k_out, v_out)):
            pieces = [nkv[l, i, d * tok:d * tok + half, :] for d in range(n)]
            pieces += [nkv[l, i, d * tok + half:(d + 1) * tok, :] for d in reversed(range(n))]
            tr[...] = jnp.concatenate(pieces, axis=0).astype(F32).T
            out[l] = tr[my_rows, :].astype(BF16)
        h_copy.wait_recv()

        acc[...] = jnp.zeros_like(acc)

        def ff(i, _):
            g = l * nff + i
            slot = lax.rem(g, SLOTS)
            cg, cu, cd = ff_copies(g)
            cg.wait()
            cu.wait()
            y = mm(h2[...], gu[slot])
            gate = y[:, :FF_CHUNK]
            act = (gate * jax.nn.sigmoid(gate) * y[:, FF_CHUNK:]).astype(BF16)
            cd.wait()
            acc[...] += mm(act, w2[slot])

            @pl.when(g + SLOTS < total_ff)
            def _():
                ff_start(g + SLOTS)
            return 0
        lax.fori_loop(0, nff, ff, 0)
        p_copy = rcopy(acc.at[sib_tok, :], part, p_sem.at[0], p_sem.at[1], sib)
        p_copy.start()
        h_copy.wait_send()
        mine = x_s[...].astype(F32) + acc[own_tok, :]
        p_copy.wait_recv()
        x_s[...] = (mine + part[...]).astype(BF16)
        p_copy.wait_send()
        return 0

    lax.fori_loop(0, L, layer, 0)
    x_out[...] = x_s[...]

    def drain(l, _):
        full = kv.at[l, :, my_rows, :]
        rcopy(full, full, ss_sib.at[l], rs_sib.at[l, 0], sib).wait_send()
        rcopy(full, full, ss_nbr.at[l], rs_nbr.at[l, 0], nbr).wait_send()
        full = kv.at[l, :, nbr_rows, :]
        rcopy(full, full, ss_fwd.at[l], rs_fwd.at[l, 0], sib).wait_send()
        return 0
    lax.fori_loop(0, L, drain, 0)


def solution(mesh):
    n = mesh.shape['cp']

    def device_fn(hidden, prefix_k, prefix_v, gain_attn, gain_mlp, w_query, w_key, w_value, w_out, w_gate, w_up, w_down):
        L, D, kvh, hd = w_key.shape
        heads = w_query.shape[2]
        tok = hidden.shape[0]
        plen = prefix_k.shape[1]
        cols = prefix_k.shape[2]
        ff = w_gate.shape[2]
        grp = heads // kvh
        half = tok // 2
        me = lax.axis_index('cp')
        pieces = jnp.stack([me, 2 * n - 1 - me])
        pos = (plen + pieces[:, None] * half + jnp.arange(half)).reshape(-1)
        inv_freq = ROPE_THETA ** (-jnp.arange(0, hd, 2, dtype=F32) / hd)
        ang = pos.astype(F32)[:, None] * inv_freq[None, :]
        cos_t = jnp.cos(ang)
        sin_t = jnp.sin(ang)
        cos2 = jnp.concatenate([cos_t, cos_t], axis=1)
        sin2 = jnp.concatenate([-sin_t, sin_t], axis=1)
        pk = prefix_k.transpose(0, 2, 1)
        pv = prefix_v.transpose(0, 2, 1)
        wq = w_query.transpose(0, 2, 1, 3)
        wkv = jnp.concatenate([w_key.reshape(L, D, kvh * hd), w_value.reshape(L, D, kvh * hd)], axis=2)
        wo = w_out.reshape(L, heads * hd, D)
        g1 = gain_attn[:, None, :]
        g2 = gain_mlp[:, None, :]
        cfg = (n, L, D, heads, kvh, hd, tok, cols, plen)
        nch = plen // COMM_CHUNK
        rows = grp * tok
        dma = pltpu.SemaphoreType.DMA
        vm = pl.BlockSpec(memory_space=pltpu.VMEM)
        hbm = pl.BlockSpec(memory_space=pl.ANY)
        hid, nk, nv = pl.pallas_call(
            functools.partial(kernel, cfg),
            out_shape=(jax.ShapeDtypeStruct((tok, D), BF16),
                       jax.ShapeDtypeStruct((L, cols, n * tok), BF16),
                       jax.ShapeDtypeStruct((L, cols, n * tok), BF16)),
            in_specs=[vm, hbm, hbm, vm, vm, hbm, hbm, hbm, hbm, hbm, hbm, vm, vm],
            out_specs=(vm, vm, vm),
            scratch_shapes=[
                pltpu.VMEM((L, 2, hd, plen), BF16),
                pltpu.VMEM((SLOTS, D, 2 * FF_CHUNK), BF16),
                pltpu.VMEM((SLOTS, FF_CHUNK, D), BF16),
                pltpu.VMEM((D, heads * hd), BF16),
                pltpu.VMEM((D, 2 * kvh * hd), BF16),
                pltpu.VMEM((heads * hd, D), BF16),
                pltpu.VMEM((L, 2, n * tok, hd), BF16),
                pltpu.VMEM((kvh, 2, tok, hd), BF16),
                pltpu.VMEM((heads * tok, hd), BF16),
                pltpu.VMEM((rows, hd), BF16),
                pltpu.VMEM((2 * tok, D), BF16),
                pltpu.VMEM((2 * tok, D), F32),
                pltpu.VMEM((tok, D), F32),
                pltpu.VMEM((tok, D), BF16),
                pltpu.VMEM((tok, grp * hd), BF16),
                pltpu.VMEM((tok, grp * hd), BF16),
                pltpu.VMEM((tok, grp * hd), BF16),
                pltpu.VMEM((2, rows, hd), F32),
                pltpu.VMEM((2, rows, hd), F32),
                pltpu.VMEM((2, rows, hd), F32),
                pltpu.VMEM((hd, n * tok), F32),
                dma((L,)), dma((L,)), dma((L,)), dma((L,)),
                dma((L, nch)), dma((L, nch)), dma((L, nch)),
                dma((n,)), dma((L, n)),
                dma((2,)), dma((2,)), dma((2,)), dma((2,)),
                dma, dma, dma, dma((SLOTS, 2)), dma((SLOTS,)),
            ],
            compiler_params=pltpu.CompilerParams(collective_id=0, has_side_effects=True, vmem_limit_bytes=67043328),
            name='prefill',
        )(hidden, pk, pv, g1, g2, wq, wkv, wo, w_gate, w_up, w_down, cos2, sin2)
        cache_k = jnp.concatenate([pk, nk], axis=2).transpose(0, 2, 1)
        cache_v = jnp.concatenate([pv, nv], axis=2).transpose(0, 2, 1)
        return hid, cache_k, cache_v

    in_specs = (P(('req', 'cp'), None), P(None, 'req', 'cp'), P(None, 'req', 'cp')) + (P(),) * 9
    out_specs = (P(('req', 'cp'), None), P(None, 'req', 'cp'), P(None, 'req', 'cp'))
    return jax.shard_map(device_fn, mesh=mesh, in_specs=in_specs, out_specs=out_specs, check_vma=False)
```

```python
import functools
import math

import jax
import jax.numpy as jnp
from jax import lax
from jax.experimental import pallas as pl
from jax.experimental.pallas import tpu as pltpu
from jax.sharding import PartitionSpec as P

NORM_EPS = 1e-5
ROPE_THETA = 500000.0
MESH = pl.DeviceIdType.MESH
F32 = jnp.float32
BF16 = jnp.bfloat16

COMM_CHUNK = 2048
KEY_CHUNK = 1024
GU_CHUNK = 512
GU_SLOTS = 6
DN_CHUNK = 256
DN_SLOTS = 6


def rms(x, gain):
    xf = x.astype(F32)
    inv = lax.rsqrt(jnp.mean(xf * xf, axis=-1, keepdims=True) + NORM_EPS)
    return (xf * inv * gain.astype(F32)).astype(BF16)


def mm(a, b):
    return jnp.dot(a, b, preferred_element_type=F32)


def mm_t(a, b):
    return lax.dot_general(a, b, (((1,), (1,)), ((), ())), preferred_element_type=F32)


def kernel(cfg, x_in, pk, pv, g1, g2, wq, wk, wv, wo, wg, wu, wd, cos_ref, sin_ref,
           x_out, k_out, v_out,
           kv, gu, w2, wq_v, wkv_v, wo_v, nkv, kvs, qs, qr, h2, act, pr, part, x_s, att_own, att_snd, att_rcv,
           m_s, l_s, o_s, tr, gains, gain_v, trig, spread, wide, newc,
           lsem, ss_sib, ss_nbr, ss_fwd, rs_sib, rs_nbr, rs_fwd, nk_s, nk_r, q_sem, o_sem, h_sem, p_send, p_recv,
           wq_sem, wkv_sem, wo_sem, gu_sem, w2_sem, in_sem, new_sem, credit):
    n, L, D, heads, kvh, hd, tok, cols, plen = cfg
    grp = heads // kvh
    per = n // kvh
    grows = grp * tok
    gcols = grp * hd
    nch = plen // COMM_CHUNK
    ff_half = wg.shape[2] // 2
    ngu = pl.cdiv(ff_half, GU_CHUNK)
    ndn = D // DN_CHUNK
    ksplit = ff_half // 2 // 256 * 256 + 256
    scale = hd ** -0.5 * math.log2(math.e)

    me = lax.axis_index('cp')
    core = lax.rem(me, 2)
    chip = lax.div(me, 2)
    kvj = lax.div(me, per)
    quarter = lax.rem(me, per)
    sib = me + 1 - 2 * core
    nbr = kvj * per + lax.rem(quarter + 2, per)
    mate = 2 * (n // 2 - 1 - chip) + core

    def rows_of(dev):
        return pl.ds(pl.multiple_of(lax.rem(dev, per) * cols, cols), cols)

    my_rows = rows_of(me)
    nbr_rows = rows_of(nbr)
    sib_rows = rows_of(sib)
    sibnbr = kvj * per + lax.rem(lax.rem(sib, per) + 2, per)
    sibnbr_rows = rows_of(sibnbr)

    def rcopy(src, dst, s, r, dev):
        return pltpu.make_async_remote_copy(src_ref=src, dst_ref=dst, send_sem=s, recv_sem=r,
                                            device_id={'cp': dev}, device_id_type=MESH)

    def cpos(ch):
        return pl.ds(ch * COMM_CHUNK if isinstance(ch, int) else pl.multiple_of(ch * COMM_CHUNK, COMM_CHUNK), COMM_CHUNK)

    def wq_start(l):
        for h in range(heads):
            pltpu.make_async_copy(wq.at[l, h], wq_v.at[:, pl.ds(h * hd, hd)], wq_sem).start()
        for i, src in enumerate((wk, wv)):
            pltpu.make_async_copy(src.at[l], wkv_v.at[:, pl.ds(i * hd, hd)], wkv_sem.at[i]).start()

    def wo_start(l):
        pltpu.make_async_copy(wo.at[l], wo_v, wo_sem).start()

    def gu_off(i):
        return pl.multiple_of(jnp.minimum(i * GU_CHUNK, ff_half - GU_CHUNK), 128)

    def gu_copies(g):
        l = lax.div(g, ngu)
        off = pl.multiple_of(core * ff_half + gu_off(lax.rem(g, ngu)), 128)
        slot = lax.rem(g, GU_SLOTS)
        return (pltpu.make_async_copy(wg.at[l, :, pl.ds(off, GU_CHUNK)], gu.at[slot, :, pl.ds(0, GU_CHUNK)], gu_sem.at[slot, 0]),
                pltpu.make_async_copy(wu.at[l, :, pl.ds(off, GU_CHUNK)], gu.at[slot, :, pl.ds(GU_CHUNK, GU_CHUNK)], gu_sem.at[slot, 1]))

    def gu_start(g):
        for c in gu_copies(g):
            c.start()

    def gu_wait(g):
        for c in gu_copies(g):
            c.wait()

    def dn_copy(g):
        l = lax.div(g, ndn)
        row = pl.multiple_of(core * ff_half, 128)
        col = pl.multiple_of(lax.rem(g, ndn) * DN_CHUNK, DN_CHUNK)
        slot = lax.rem(g, DN_SLOTS)
        return pltpu.make_async_copy(wd.at[l, pl.ds(row, ff_half), pl.ds(col, DN_CHUNK)], w2.at[slot], w2_sem.at[slot])

    def own_local(l):
        b = lax.rem(l, 2)
        pltpu.make_async_copy(pk.at[l], kv.at[b, 0, my_rows, :], lsem.at[l]).start()
        pltpu.make_async_copy(pv.at[l], kv.at[b, 1, my_rows, :], lsem.at[l]).start()

    def own_send(l):
        b = lax.rem(l, 2)

        def body(ch, _):
            for i, src in enumerate((pk, pv)):
                rcopy(src.at[l, :, cpos(ch)], kv.at[b, i, my_rows, cpos(ch)], ss_nbr.at[l], rs_nbr.at[l, ch], nbr).start()
                rcopy(src.at[l, :, cpos(ch)], kv.at[b, i, my_rows, cpos(ch)], ss_sib.at[l], rs_sib.at[l, ch], sib).start()
            return 0
        lax.fori_loop(0, nch, body, 0)

    def forward(l, ch):
        blk = kv.at[lax.rem(l, 2), :, nbr_rows, cpos(ch)]
        rcopy(blk, blk, ss_nbr.at[l], rs_nbr.at[l, ch], nbr).wait_recv()
        rcopy(blk, blk, ss_fwd.at[l], rs_fwd.at[l, ch], sib).start()

    def chunk_ready(l, ch):
        @pl.when(ch + 1 < nch)
        def _():
            forward(l, ch + 1)
        blk = kv.at[lax.rem(l, 2), :, sib_rows, cpos(ch)]
        rcopy(blk, blk, ss_sib.at[l], rs_sib.at[l, ch], sib).wait_recv()
        blk = kv.at[lax.rem(l, 2), :, sibnbr_rows, cpos(ch)]
        rcopy(blk, blk, ss_fwd.at[l], rs_fwd.at[l, ch], sib).wait_recv()

    def kv_free(l):
        full = kv.at[lax.rem(l, 2), :, nbr_rows, :]
        rcopy(full, full, ss_fwd.at[l], rs_fwd.at[l, 0], sib).wait_send()

        @pl.when(l + 2 < L)
        def _():
            pl.semaphore_signal(credit.at[0], inc=1, device_id={'cp': nbr}, device_id_type=MESH)
            pl.semaphore_signal(credit.at[1], inc=1, device_id={'cp': sib}, device_id_type=MESH)
            own_local(l + 2)

    barrier = pltpu.get_barrier_semaphore()
    for off in range(1, n):
        pl.semaphore_signal(barrier, inc=1, device_id={'cp': lax.rem(me + off, n)}, device_id_type=MESH)

    small = [pltpu.make_async_copy(src, dst, in_sem.at[i]) for i, (src, dst) in enumerate(
        ((x_in, x_s), (g1, gain_v.at[0]), (g2, gain_v.at[1]), (cos_ref, trig.at[0]), (sin_ref, trig.at[1])))]
    for c in small:
        c.start()
    wq_start(0)
    pl.semaphore_wait(barrier, n - 1)
    own_send(0)
    own_local(0)
    wo_start(0)

    def prime_gu(g, _):
        gu_start(g)
        return 0
    lax.fori_loop(0, GU_SLOTS, prime_gu, 0)

    def prime_dn(g, _):
        dn_copy(g).start()
        return 0
    lax.fori_loop(0, DN_SLOTS, prime_dn, 0)

    own_local(1)

    src_row = lax.broadcasted_iota(jnp.int32, (hd, kvh * kvh * hd), 0)
    dst_col = lax.broadcasted_iota(jnp.int32, (hd, kvh * kvh * hd), 1)
    spread[...] = jnp.where(dst_col == src_row * kvh + lax.div(dst_col, kvh * hd) * (kvh * hd + 1), 1.0, 0.0).astype(BF16)
    for c in small:
        c.wait()
    for i in range(2):
        gain = gain_v[i].astype(F32)
        for l in range(L):
            gains[i, l] = gain[l:l + 1, :]

    def token_pos(t, dev):
        half = tok // 2
        return jnp.where(t < half, dev * half + t, (2 * n - 1 - dev) * half + t - half)

    def reset(st):
        m_s[st] = jnp.full((grows, hd), -jnp.inf, F32)
        l_s[st] = jnp.zeros((grows, hd), F32)
        o_s[st] = jnp.zeros((grows, hd), F32)

    def fold(st, s, pv_dot):
        width = s.shape[1]
        m_prev = m_s[st]
        m_new = jnp.maximum(m_prev, jnp.max(s, axis=1, keepdims=True))
        alpha = jnp.exp2((m_prev - m_new) * scale)
        p = jnp.exp2((s - jnp.concatenate([m_new] * (width // hd), axis=1)) * scale)
        lsum = p[:, :hd]
        for b in range(1, width // hd):
            lsum = lsum + p[:, b * hd:(b + 1) * hd]
        m_s[st] = m_new
        l_s[st] = alpha * l_s[st] + lsum
        o_s[st] = alpha * o_s[st] + pv_dot(p.astype(BF16))

    def attend_prefix(l, st, q_at, ch):
        subs = [pl.ds(pl.multiple_of(ch * COMM_CHUNK + sub * KEY_CHUNK, KEY_CHUNK), KEY_CHUNK)
                for sub in range(COMM_CHUNK // KEY_CHUNK)]
        scores = [mm(q_at(), kv[lax.rem(l, 2), 0, :, pos]) for pos in subs]
        for s, pos in zip(scores, subs):
            fold(st, s, lambda p: mm_t(p, kv[lax.rem(l, 2), 1, :, pos]))

    def attend_new(l, st, q_at, dev):
        s = mm_t(q_at(), nkv[l, 0])
        width = n * tok
        tq = lax.broadcasted_iota(jnp.int32, (grows, width), 0) & (tok - 1)
        col = lax.broadcasted_iota(jnp.int32, (grows, width), 1)
        tk = col & (tok - 1)
        dk = col >> (tok.bit_length() - 1)
        allowed = token_pos(tk, dk) <= token_pos(tq, dev)
        s = jnp.where(allowed, s, -jnp.inf)
        fold(st, s, lambda p: mm(p, nkv[l, 1]))

    def finish(st, dst):
        o = (o_s[st] / jnp.sum(l_s[st], axis=1, keepdims=True)).astype(BF16)
        for h in range(grp):
            dst[:, h * hd:(h + 1) * hd] = o[h * tok:(h + 1) * tok, :]

    own_q = pl.ds(pl.multiple_of(kvj * grows, grows), grows)
    mate_q = pl.ds(pl.multiple_of((1 - kvj) * grows, grows), grows)
    own_tok = pl.ds(pl.multiple_of(core * tok, tok), tok)
    sib_tok = pl.ds(pl.multiple_of((1 - core) * tok, tok), tok)
    my_new = pl.ds(pl.multiple_of(me * tok, tok), tok)

    def layer(l, _):
        @pl.when(l > 0)
        def _():
            forward(l, 0)
        h = rms(x_s[...], gains[0, l])
        pltpu.make_async_copy(wo.at[l], wq_v, wq_sem).wait()
        cos_t = jnp.concatenate([trig[0], trig[0]], axis=1)
        sin_t = jnp.concatenate([-trig[1], trig[1]], axis=1)

        def rope(z):
            return (z * cos_t + pltpu.roll(z, hd // 2, 1) * sin_t).astype(BF16)

        def project_q(g):
            for pair in range(grp // 2):
                y = mm(h, wq_v[:, pl.ds(pl.multiple_of(g * gcols + 2 * pair * hd, hd), 2 * hd)])
                for s in range(2):
                    row = pl.multiple_of(g * grows + (2 * pair + s) * tok, tok)
                    qs[pl.ds(row, tok), :] = rope(y[:, s * hd:(s + 1) * hd])

        project_q(1 - kvj)
        q_copy = rcopy(qs.at[mate_q, :], qr, q_sem.at[0], q_sem.at[1], mate)
        q_copy.start()
        project_q(kvj)
        hs = jnp.concatenate([h[:, b * hd:(b + 1) * hd] for b in range(D // hd)], axis=0)
        hs = mm(hs, spread[...]).astype(BF16)
        for b in range(D // hd):
            for j in range(kvh):
                wide[j * tok:(j + 1) * tok, b * kvh * hd:(b + 1) * kvh * hd] = hs[b * tok:(b + 1) * tok, j * kvh * hd:(j + 1) * kvh * hd]
        for i, src in enumerate((wk, wv)):
            pltpu.make_async_copy(src.at[l], wkv_v.at[:, pl.ds(i * hd, hd)], wkv_sem.at[i]).wait()
        y = mm(wide[...], wkv_v[...])
        for j in range(kvh):
            kvs[j, 0] = rope(y[j * tok:(j + 1) * tok, :hd])
            kvs[j, 1] = y[j * tok:(j + 1) * tok, hd:].astype(BF16)

        @pl.when(l + 1 < L)
        def _():
            wq_start(l + 1)

        for i in range(2):
            nkv[l, i, my_new, :] = kvs[kvj, i]

        def nk_copy(off):
            dst = lax.rem(me + off, n)
            return rcopy(kvs.at[lax.div(dst, per)], nkv.at[l, :, my_new, :], nk_s.at[off], nk_r.at[l, me], dst)


        @pl.when(l == 0)
        def _():
            forward(l, 0)
        full = kv.at[lax.rem(l, 2), :, my_rows, :]
        pltpu.make_async_copy(full, full, lsem.at[l]).wait()

        reset(0)
        reset(1)

        def own_chunk(ch, _):
            attend_prefix(l, 0, lambda: qs[own_q, :], ch)
            return 0

        def first_half(ch, _):
            chunk_ready(l, ch)

            @pl.when(ch == nch // 2 - 1)
            def _():
                for off in range(1, n):
                    nk_copy(off).start()

                @pl.when((l > 0) & (l + 1 < L))
                def _():
                    pl.semaphore_wait(credit.at[0], 1)
                    pl.semaphore_wait(credit.at[1], 1)

                @pl.when(l + 1 < L)
                def _():
                    own_send(l + 1)
            return own_chunk(ch, 0)
        lax.fori_loop(0, nch // 2, first_half, 0)
        q_copy.wait_recv()

        def mate_chunk(ch, _):
            @pl.when(ch >= nch // 2)
            def _():
                chunk_ready(l, ch)
            attend_prefix(l, 1, lambda: qr[...], ch)
            return 0
        lax.fori_loop(0, nch, mate_chunk, 0)
        for off in range(1, n):
            src = lax.rem(me + off, n)
            blk = nkv.at[l, :, pl.ds(pl.multiple_of(src * tok, tok), tok), :]
            rcopy(blk, blk, nk_s.at[off], nk_r.at[l, src], src).wait_recv()
        attend_new(l, 1, lambda: qr[...], mate)
        finish(1, att_snd)
        o_copy = rcopy(att_snd, att_rcv, o_sem.at[0], o_sem.at[1], mate)
        o_copy.start()
        lax.fori_loop(nch // 2, nch, own_chunk, 0)
        attend_new(l, 0, lambda: qs[own_q, :], me)
        finish(0, att_own)
        kv_free(l)

        pltpu.make_async_copy(wo.at[l], wo_v, wo_sem).wait()
        y = mm(att_own[...], wo_v[pl.ds(pl.multiple_of(kvj * gcols, gcols), gcols), :])
        o_copy.wait_recv()
        y = y + mm(att_rcv[...], wo_v[pl.ds(pl.multiple_of((1 - kvj) * gcols, gcols), gcols), :])
        x1 = (x_s[...].astype(F32) + y).astype(BF16)
        x_s[...] = x1
        h2[own_tok, :] = rms(x1, gains[1, l])
        h_copy = rcopy(h2.at[own_tok, :], h2.at[own_tok, :], h_sem.at[0], h_sem.at[1], sib)
        h_copy.start()

        q_copy.wait_send()
        o_copy.wait_send()
        for off in range(1, n):
            nk_copy(off).wait_send()
        half = tok // 2
        for i, out in enumerate((k_out, v_out)):
            pieces = [nkv[l, i, d * tok:d * tok + half, :] for d in range(n)]
            pieces += [nkv[l, i, d * tok + half:(d + 1) * tok, :] for d in reversed(range(n))]
            tr[...] = jnp.concatenate(pieces, axis=0).astype(F32).T
            newc[l, i] = tr[my_rows, :].astype(BF16)
            pltpu.make_async_copy(newc.at[l, i], out.at[l], new_sem.at[i]).start()
        h_copy.wait_recv()

        def gate_up(i):
            return mm(h2[...], gu[lax.rem(l * ngu + i, GU_SLOTS)])

        def activate(i, y):
            gate = y[:, :GU_CHUNK]
            act[:, pl.ds(gu_off(i), GU_CHUNK)] = (gate * jax.nn.sigmoid(gate) * y[:, GU_CHUNK:]).astype(BF16)

        def refill(i):
            @pl.when(l * ngu + i + GU_SLOTS < L * ngu)
            def _():
                gu_start(l * ngu + i + GU_SLOTS)

        gu_wait(l * ngu)
        activate(0, gate_up(0))
        refill(0)

        def gu_pair(k, _):
            gu_wait(l * ngu + 2 * k + 1)
            gu_wait(l * ngu + 2 * k + 2)
            ya = gate_up(2 * k + 1)
            yb = gate_up(2 * k + 2)
            activate(2 * k + 1, ya)
            activate(2 * k + 2, yb)
            refill(2 * k + 1)
            refill(2 * k + 2)
            return 0
        lax.fori_loop(0, (ngu - 1) // 2, gu_pair, 0)

        @pl.when(l + 1 < L)
        def _():
            wo_start(l + 1)

        def p_copy(i):
            return rcopy(pr.at[i, sib_tok, :], part.at[i], p_send.at[i], p_recv.at[i], sib)

        def down(k, _):
            for i in (2 * k, 2 * k + 1):
                dn_copy(l * ndn + i).wait()
            for i in (2 * k, 2 * k + 1):
                slot = lax.rem(l * ndn + i, DN_SLOTS)
                pr[i] = mm(act[:, :ksplit], w2[slot, :ksplit, :]) + mm(act[:, ksplit:], w2[slot, ksplit:, :])
            for i in (2 * k, 2 * k + 1):
                p_copy(i).start()

                @pl.when(l * ndn + i + DN_SLOTS < L * ndn)
                def _():
                    dn_copy(l * ndn + i + DN_SLOTS).start()
            return 0
        lax.fori_loop(0, ndn // 2, down, 0)
        h_copy.wait_send()
        for i in range(ndn):
            cs = slice(i * DN_CHUNK, (i + 1) * DN_CHUNK)
            mine = x_s[:, cs].astype(F32) + pr[i, own_tok, :]
            p_copy(i).wait_recv()
            x_s[:, cs] = (mine + part[i]).astype(BF16)
            p_copy(i).wait_send()
        return 0

    lax.fori_loop(0, L, layer, 0)
    out_copy = pltpu.make_async_copy(x_s, x_out, in_sem.at[0])
    out_copy.start()
    for i, out in enumerate((k_out, v_out)):
        pltpu.make_async_copy(newc.at[:, i], out, new_sem.at[i]).wait()

    def drain(l, _):
        full = kv.at[lax.rem(l, 2), :, my_rows, :]
        rcopy(full, full, ss_sib.at[l], rs_sib.at[l, 0], sib).wait_send()
        rcopy(full, full, ss_nbr.at[l], rs_nbr.at[l, 0], nbr).wait_send()
        return 0
    lax.fori_loop(0, L, drain, 0)
    out_copy.wait()


def solution(mesh):
    n = mesh.shape['cp']

    def device_fn(hidden, prefix_k, prefix_v, gain_attn, gain_mlp, w_query, w_key, w_value, w_out, w_gate, w_up, w_down):
        L, D, kvh, hd = w_key.shape
        heads = w_query.shape[2]
        tok = hidden.shape[0]
        plen = prefix_k.shape[1]
        cols = prefix_k.shape[2]
        ff = w_gate.shape[2]
        grp = heads // kvh
        half = tok // 2
        me = lax.axis_index('cp')
        pieces = jnp.stack([me, 2 * n - 1 - me])
        pos = (plen + pieces[:, None] * half + jnp.arange(half)).reshape(-1)
        inv_freq = ROPE_THETA ** (-jnp.arange(0, hd, 2, dtype=F32) / hd)
        ang = pos.astype(F32)[:, None] * inv_freq[None, :]
        cos_t = jnp.cos(ang)
        sin_t = jnp.sin(ang)
        pk = prefix_k.transpose(0, 2, 1)
        pv = prefix_v.transpose(0, 2, 1)
        wq = w_query.transpose(0, 2, 1, 3)
        wk = w_key.reshape(L, D * kvh, hd)
        wv = w_value.reshape(L, D * kvh, hd)
        wo = w_out.reshape(L, heads * hd, D)
        cfg = (n, L, D, heads, kvh, hd, tok, cols, plen)
        nch = plen // COMM_CHUNK
        rows = grp * tok
        dma = pltpu.SemaphoreType.DMA
        hbm = pl.BlockSpec(memory_space=pl.ANY)
        hid, nk, nv = pl.pallas_call(
            functools.partial(kernel, cfg),
            out_shape=(jax.ShapeDtypeStruct((tok, D), BF16),
                       jax.ShapeDtypeStruct((L, cols, n * tok), BF16),
                       jax.ShapeDtypeStruct((L, cols, n * tok), BF16)),
            in_specs=[hbm] * 14,
            out_specs=(hbm, hbm, hbm),
            scratch_shapes=[
                pltpu.VMEM((2, 2, hd, plen), BF16),
                pltpu.VMEM((GU_SLOTS, D, 2 * GU_CHUNK), BF16),
                pltpu.VMEM((DN_SLOTS, ff // 2, DN_CHUNK), BF16),
                pltpu.VMEM((D, heads * hd), BF16),
                pltpu.VMEM((D * kvh, 2 * hd), BF16),
                pltpu.VMEM((heads * hd, D), BF16),
                pltpu.VMEM((L, 2, n * tok, hd), BF16),
                pltpu.VMEM((kvh, 2, tok, hd), BF16),
                pltpu.VMEM((heads * tok, hd), BF16),
                pltpu.VMEM((rows, hd), BF16),
                pltpu.VMEM((2 * tok, D), BF16),
                pltpu.VMEM((2 * tok, ff // 2), BF16),
                pltpu.VMEM((D // DN_CHUNK, 2 * tok, DN_CHUNK), F32),
                pltpu.VMEM((D // DN_CHUNK, tok, DN_CHUNK), F32),
                pltpu.VMEM((tok, D), BF16),
                pltpu.VMEM((tok, grp * hd), BF16),
                pltpu.VMEM((tok, grp * hd), BF16),
                pltpu.VMEM((tok, grp * hd), BF16),
                pltpu.VMEM((2, rows, hd), F32),
                pltpu.VMEM((2, rows, hd), F32),
                pltpu.VMEM((2, rows, hd), F32),
                pltpu.VMEM((hd, n * tok), F32),
                pltpu.VMEM((2, L, 1, D), F32),
                pltpu.VMEM((2, L, D), BF16),
                pltpu.VMEM((2, tok, hd // 2), F32),
                pltpu.VMEM((hd, kvh * kvh * hd), BF16),
                pltpu.VMEM((kvh * tok, D * kvh), BF16),
                pltpu.VMEM((L, 2, cols, n * tok), BF16),
                dma((L,)), dma((L,)), dma((L,)), dma((L,)),
                dma((L, nch)), dma((L, nch)), dma((L, nch)),
                dma((n,)), dma((L, n)),
                dma((2,)), dma((2,)), dma((2,)), dma((D // DN_CHUNK,)), dma((D // DN_CHUNK,)),
                dma, dma((2,)), dma, dma((GU_SLOTS, 2)), dma((DN_SLOTS,)), dma((5,)), dma((2,)), pltpu.SemaphoreType.REGULAR((2,)),
            ],
            compiler_params=pltpu.CompilerParams(collective_id=0, has_side_effects=True, vmem_limit_bytes=67043328),
            name='prefill',
        )(hidden, pk, pv, gain_attn, gain_mlp, wq, wk, wv, wo, w_gate, w_up, w_down, cos_t, sin_t)
        cache_k = jnp.concatenate([pk, nk], axis=2).transpose(0, 2, 1)
        cache_v = jnp.concatenate([pv, nv], axis=2).transpose(0, 2, 1)
        return hid, cache_k, cache_v

    in_specs = (P(('req', 'cp'), None), P(None, 'req', 'cp'), P(None, 'req', 'cp')) + (P(),) * 9
    out_specs = (P(('req', 'cp'), None), P(None, 'req', 'cp'), P(None, 'req', 'cp'))
    return jax.shard_map(device_fn, mesh=mesh, in_specs=in_specs, out_specs=out_specs, check_vma=False)
```

```python
import functools
import math

import jax
import jax.numpy as jnp
from jax import lax
from jax.experimental import pallas as pl
from jax.experimental.pallas import tpu as pltpu
from jax.sharding import PartitionSpec as P

NORM_EPS = 1e-5
ROPE_THETA = 500000.0
MESH = pl.DeviceIdType.MESH
F32 = jnp.float32
BF16 = jnp.bfloat16

COMM_CHUNK = 1024
KEY_CHUNK = 512
LOOKAHEAD = 2
GU_CHUNK = 512
GU_UNROLL = 3
GU_SLOTS = 7
DN_CHUNK = 256
DN_SLOTS = 6


def rms(x, gain):
    xf = x.astype(F32)
    inv = lax.rsqrt(jnp.mean(xf * xf, axis=-1, keepdims=True) + NORM_EPS)
    return (xf * inv * gain.astype(F32)).astype(BF16)


def mm(a, b):
    return jnp.dot(a, b, preferred_element_type=F32)


def mm_t(a, b):
    return lax.dot_general(a, b, (((1,), (1,)), ((), ())), preferred_element_type=F32)


def kernel(cfg, x_in, pk, pv, g1, g2, wq, wk, wv, wo, wg, wu, wd, cos_ref, sin_ref,
           x_out, k_out, v_out,
           kv, gu, w2, wq_v, wkv_v, wo_v, nkv, kvs, qs, qr, h2, act, pr, part, x_s, att_own, att_snd, att_rcv,
           m_s, l_s, o_s, tr, gains, gain_v, trig, spread, newc,
           lsem, ss_sib, ss_nbr, ss_fwd, rs_sib, rs_nbr, rs_fwd, nk_s, nk_f, nk_r, q_sem, o_sem, h_sem, p_send, p_recv,
           wq_sem, wkv_sem, wo_sem, gu_sem, w2_sem, in_sem, new_sem, credit):
    n, L, D, heads, kvh, hd, tok, cols, plen = cfg
    grp = heads // kvh
    per = n // kvh
    grows = grp * tok
    gcols = grp * hd
    nch = plen // COMM_CHUNK
    ff_half = wg.shape[2] // 2
    ngu = pl.cdiv(ff_half, GU_CHUNK)
    ndn = D // DN_CHUNK
    ksplit = ff_half // 2 // 256 * 256 + 256
    scale = hd ** -0.5 * math.log2(math.e)

    me = lax.axis_index('cp')
    core = lax.rem(me, 2)
    chip = lax.div(me, 2)
    kvj = lax.div(me, per)
    quarter = lax.rem(me, per)
    sib = me + 1 - 2 * core
    nbr = kvj * per + lax.rem(quarter + 2, per)
    mate = 2 * (n // 2 - 1 - chip) + core

    def rows_of(dev):
        return pl.ds(pl.multiple_of(lax.rem(dev, per) * cols, cols), cols)

    my_rows = rows_of(me)
    nbr_rows = rows_of(nbr)
    sib_rows = rows_of(sib)
    sibnbr = kvj * per + lax.rem(lax.rem(sib, per) + 2, per)
    sibnbr_rows = rows_of(sibnbr)

    def rcopy(src, dst, s, r, dev):
        return pltpu.make_async_remote_copy(src_ref=src, dst_ref=dst, send_sem=s, recv_sem=r,
                                            device_id={'cp': dev}, device_id_type=MESH)

    def cpos(ch):
        return pl.ds(ch * COMM_CHUNK if isinstance(ch, int) else pl.multiple_of(ch * COMM_CHUNK, COMM_CHUNK), COMM_CHUNK)

    def wq_start(l):
        for h in range(heads):
            pltpu.make_async_copy(wq.at[l, h], wq_v.at[:, pl.ds(h * hd, hd)], wq_sem).start()
        for i, src in enumerate((wk, wv)):
            pltpu.make_async_copy(src.at[l], wkv_v.at[:, pl.ds(i * hd, hd)], wkv_sem.at[i]).start()

    def wo_start(l):
        pltpu.make_async_copy(wo.at[l], wo_v, wo_sem).start()

    def gu_off(i):
        return pl.multiple_of(jnp.minimum(i * GU_CHUNK, ff_half - GU_CHUNK), 128)

    def gu_copies(g):
        l = lax.div(g, ngu)
        off = pl.multiple_of(core * ff_half + gu_off(lax.rem(g, ngu)), 128)
        slot = lax.rem(g, GU_SLOTS)
        return (pltpu.make_async_copy(wg.at[l, :, pl.ds(off, GU_CHUNK)], gu.at[slot, :, pl.ds(0, GU_CHUNK)], gu_sem.at[slot, 0]),
                pltpu.make_async_copy(wu.at[l, :, pl.ds(off, GU_CHUNK)], gu.at[slot, :, pl.ds(GU_CHUNK, GU_CHUNK)], gu_sem.at[slot, 1]))

    def gu_start(g):
        for c in gu_copies(g):
            c.start()

    def gu_wait(g):
        for c in gu_copies(g):
            c.wait()

    def dn_copy(g):
        l = lax.div(g, ndn)
        row = pl.multiple_of(core * ff_half, 128)
        col = pl.multiple_of(lax.rem(g, ndn) * DN_CHUNK, DN_CHUNK)
        slot = lax.rem(g, DN_SLOTS)
        return pltpu.make_async_copy(wd.at[l, pl.ds(row, ff_half), pl.ds(col, DN_CHUNK)], w2.at[slot], w2_sem.at[slot])

    def own_local(l):
        b = lax.rem(l, 2)
        pltpu.make_async_copy(pk.at[l], kv.at[b, 0, my_rows, :], lsem.at[l]).start()
        pltpu.make_async_copy(pv.at[l], kv.at[b, 1, my_rows, :], lsem.at[l]).start()

    def own_send(l):
        b = lax.rem(l, 2)

        def body(ch, _):
            for i, src in enumerate((pk, pv)):
                rcopy(src.at[l, :, cpos(ch)], kv.at[b, i, my_rows, cpos(ch)], ss_nbr.at[l], rs_nbr.at[l, ch], nbr).start()
            return 0
        lax.fori_loop(0, nch, body, 0)
        for i, src in enumerate((pk, pv)):
            rcopy(src.at[l], kv.at[b, i, my_rows, :], ss_sib.at[l], rs_sib.at[l], sib).start()

    def forward(l, ch):
        blk = kv.at[lax.rem(l, 2), :, nbr_rows, cpos(ch)]
        rcopy(blk, blk, ss_nbr.at[l], rs_nbr.at[l, ch], nbr).wait_recv()
        rcopy(blk, blk, ss_fwd.at[l], rs_fwd.at[l, ch], sib).start()

    def chunk_wait(l, ch):
        blk = kv.at[lax.rem(l, 2), :, sibnbr_rows, cpos(ch)]
        rcopy(blk, blk, ss_fwd.at[l], rs_fwd.at[l, ch], sib).wait_recv()

    def forward_next(l, ch):
        @pl.when(l + 1 < L)
        def _():
            forward(l + 1, ch)

    def kv_free(l):
        full = kv.at[lax.rem(l, 2), :, nbr_rows, :]
        rcopy(full, full, ss_fwd.at[l], rs_fwd.at[l, 0], sib).wait_send()

        @pl.when(l + 2 < L)
        def _():
            pl.semaphore_signal(credit.at[0], inc=1, device_id={'cp': nbr}, device_id_type=MESH)
            pl.semaphore_signal(credit.at[1], inc=1, device_id={'cp': sib}, device_id_type=MESH)
            own_local(l + 2)

    barrier = pltpu.get_barrier_semaphore()
    for off in range(1, n):
        pl.semaphore_signal(barrier, inc=1, device_id={'cp': lax.rem(me + off, n)}, device_id_type=MESH)

    small = [pltpu.make_async_copy(src, dst, in_sem.at[i]) for i, (src, dst) in enumerate(
        ((x_in, x_s), (g1, gain_v.at[0]), (g2, gain_v.at[1]), (cos_ref, trig.at[0]), (sin_ref, trig.at[1])))]
    for c in small:
        c.start()
    wq_start(0)
    pl.semaphore_wait(barrier, n - 1)
    own_send(0)
    own_local(0)
    wo_start(0)

    def prime_gu(g, _):
        gu_start(g)
        return 0
    lax.fori_loop(0, GU_SLOTS, prime_gu, 0)

    def prime_dn(g, _):
        dn_copy(g).start()
        return 0
    lax.fori_loop(0, DN_SLOTS, prime_dn, 0)

    own_local(1)

    src_row = lax.broadcasted_iota(jnp.int32, (hd, kvh * kvh * hd), 0)
    dst_col = lax.broadcasted_iota(jnp.int32, (hd, kvh * kvh * hd), 1)
    spread[...] = jnp.where(dst_col == src_row * kvh + lax.div(dst_col, kvh * hd) * (kvh * hd + 1), 1.0, 0.0).astype(BF16)
    for c in small:
        c.wait()
    for i in range(2):
        gain = gain_v[i].astype(F32)
        for l in range(L):
            gains[i, l] = gain[l:l + 1, :]

    def token_pos(t, dev):
        half = tok // 2
        return jnp.where(t < half, dev * half + t, (2 * n - 1 - dev) * half + t - half)

    def reset(st):
        m_s[st] = jnp.full((grows, hd), -jnp.inf, F32)
        l_s[st] = jnp.zeros((grows, hd), F32)
        o_s[st] = jnp.zeros((grows, hd), F32)

    def fold(st, at, s, pv_dot):
        width = s.shape[1]
        m_prev = m_s[st, at, :]
        m_new = jnp.maximum(m_prev, jnp.max(s, axis=1, keepdims=True))
        alpha = jnp.exp2((m_prev - m_new) * scale)
        p = jnp.exp2((s - jnp.concatenate([m_new] * (width // hd), axis=1)) * scale)
        lsum = p[:, :hd]
        for b in range(1, width // hd):
            lsum = lsum + p[:, b * hd:(b + 1) * hd]
        m_s[st, at, :] = m_new
        l_s[st, at, :] = alpha * l_s[st, at, :] + lsum
        o_s[st, at, :] = alpha * o_s[st, at, :] + pv_dot(p.astype(BF16))

    def sweep(l, jobs):
        b = lax.rem(l, 2)

        def keys(first):
            return pl.ds(first if isinstance(first, int) else pl.multiple_of(first, KEY_CHUNK), KEY_CHUNK)

        def score(job):
            _, at, q, first, dev = job
            if first is not None:
                return mm(q(), kv[b, 0, :, keys(first)])
            s = mm_t(q(), nkv[lax.rem(l, 2), 0])
            width = n * tok
            shape = (at.stop - at.start, width)
            tq = lax.broadcasted_iota(jnp.int32, shape, 0) & (tok - 1)
            col = lax.broadcasted_iota(jnp.int32, shape, 1)
            tk = col & (tok - 1)
            dk = col >> (tok.bit_length() - 1)
            return jnp.where(token_pos(tk, dk) <= token_pos(tq, dev), s, -jnp.inf)

        def mix(job):
            if job[3] is not None:
                return lambda p: mm_t(p, kv[b, 1, :, keys(job[3])])
            return lambda p: mm(p, nkv[lax.rem(l, 2), 1])

        ahead = [score(job) for job in jobs[:LOOKAHEAD]]
        for i, job in enumerate(jobs):
            fold(job[0], job[1], ahead.pop(0), mix(job))
            if i + LOOKAHEAD < len(jobs):
                ahead.append(score(jobs[i + LOOKAHEAD]))

    def finish(st, dst, first, last):
        o = (o_s[st, first * tok:last * tok, :] / jnp.sum(l_s[st, first * tok:last * tok, :], axis=1, keepdims=True)).astype(BF16)
        for h in range(first, last):
            dst[:, h * hd:(h + 1) * hd] = o[(h - first) * tok:(h - first + 1) * tok, :]

    own_q = pl.ds(pl.multiple_of(kvj * grows, grows), grows)
    own_tok = pl.ds(pl.multiple_of(core * tok, tok), tok)
    sib_tok = pl.ds(pl.multiple_of((1 - core) * tok, tok), tok)
    my_new = pl.ds(pl.multiple_of(me * tok, tok), tok)

    def layer(l, _):
        h = rms(x_s[...], gains[0, l])
        pltpu.make_async_copy(wo.at[l], wq_v, wq_sem).wait()
        cos_t = jnp.concatenate([trig[0], trig[0]], axis=1)
        sin_t = jnp.concatenate([-trig[1], trig[1]], axis=1)

        def rope(z):
            return (z * cos_t + pltpu.roll(z, hd // 2, 1) * sin_t).astype(BF16)

        def q_copy(pair):
            at = pl.ds(pl.multiple_of((1 - kvj) * grows + 2 * pair * tok, 2 * tok), 2 * tok)
            return rcopy(qs.at[at, :], qr.at[pl.ds(2 * pair * tok, 2 * tok), :], q_sem.at[0, pair], q_sem.at[1, pair], mate)

        def project_q(g, send):
            for pair in range(grp // 2):
                y = mm(h, wq_v[:, pl.ds(pl.multiple_of(g * gcols + 2 * pair * hd, hd), 2 * hd)])
                for s in range(2):
                    row = pl.multiple_of(g * grows + (2 * pair + s) * tok, tok)
                    qs[pl.ds(row, tok), :] = rope(y[:, s * hd:(s + 1) * hd])
                if send:
                    q_copy(pair).start()

        project_q(1 - kvj, True)
        project_q(kvj, False)
        hs = jnp.concatenate([h[:, b * hd:(b + 1) * hd] for b in range(D // hd)], axis=0)
        hs = mm(hs, spread[...]).astype(BF16)
        for b in range(D // hd):
            for j in range(kvh):
                act[j * tok:(j + 1) * tok, b * kvh * hd:(b + 1) * kvh * hd] = hs[b * tok:(b + 1) * tok, j * kvh * hd:(j + 1) * kvh * hd]
        for i, src in enumerate((wk, wv)):
            pltpu.make_async_copy(src.at[l], wkv_v.at[:, pl.ds(i * hd, hd)], wkv_sem.at[i]).wait()
        y = mm(act[:kvh * tok, :kvh * D], wkv_v[...])
        for j in range(kvh):
            kvs[j, 0] = rope(y[j * tok:(j + 1) * tok, :hd])
            kvs[j, 1] = y[j * tok:(j + 1) * tok, hd:].astype(BF16)

        @pl.when(l + 1 < L)
        def _():
            wq_start(l + 1)

        for i in range(2):
            nkv[lax.rem(l, 2), i, my_new, :] = kvs[kvj, i]

        def new_rows(src):
            return nkv.at[lax.rem(l, 2), :, pl.ds(pl.multiple_of(src * tok, tok), tok), :]

        def nk_copy(k):
            dst = lax.rem(me + 2 * k, n) if k else sib
            return rcopy(kvs.at[lax.div(dst, per)], nkv.at[lax.rem(l, 2), :, my_new, :], nk_s.at[k], nk_r.at[l, me], dst)

        def nk_relay(k):
            src = lax.rem(me + 2 * k, n)
            return rcopy(new_rows(src), new_rows(src), nk_f.at[k], nk_r.at[l, src], sib)

        def relay_new():
            for k in range(1, n // 2):
                src = lax.rem(me + 2 * k, n)
                rcopy(new_rows(src), new_rows(src), nk_s.at[k], nk_r.at[l, src], src).wait_recv()
                nk_relay(k).start()

        def new_ready():
            for k in range(n // 2):
                src = lax.rem(sib + 2 * k, n)
                rcopy(new_rows(src), new_rows(src), nk_s.at[k], nk_r.at[l, src], sib).wait_recv()

        for k in range(n // 2):
            nk_copy(k).start()

        @pl.when((l > 0) & (l + 1 < L))
        def _():
            pl.semaphore_wait(credit.at[0], 1)
            pl.semaphore_wait(credit.at[1], 1)

        @pl.when(l + 1 < L)
        def _():
            own_send(l + 1)

        full = kv.at[lax.rem(l, 2), :, my_rows, :]
        pltpu.make_async_copy(full, full, lsem.at[l]).wait()
        full = kv.at[lax.rem(l, 2), :, sib_rows, :]
        rcopy(full, full, ss_sib.at[l], rs_sib.at[l], sib).wait_recv()
        reset(0)
        reset(1)
        halves = (0, grp // 2, grp)

        def o_copy(i):
            at = pl.ds(halves[i] * hd, (halves[i + 1] - halves[i]) * hd)
            return rcopy(att_snd.at[:, at], att_rcv.at[:, at], o_sem.at[0, i], o_sem.at[1, i], mate)

        def own_job(first):
            return (0, slice(0, grows), lambda: qs[own_q, :], first, me)

        def mate_job(first, at=slice(0, grows)):
            return (1, at, lambda: qr[at, :], first, mate)

        def blocks(first, last):
            return [first + k * KEY_CHUNK for k in range((last - first) // KEY_CHUNK)]

        def mate_tail(firsts):
            for i in range(2):
                at = slice(halves[i] * tok, halves[i + 1] * tok)
                sweep(l, [mate_job(f, at) for f in firsts] + [mate_job(None, at)])
                finish(1, att_snd, halves[i], halves[i + 1])
                o_copy(i).start()

        @pl.when(l == 0)
        def _():
            for pair in range(grp // 2):
                q_copy(pair).wait_recv()

            def arrive(ch, _):
                forward(l, ch)
                chunk_wait(l, ch)
                first = ch * COMM_CHUNK
                firsts = [first + k * KEY_CHUNK for k in range(COMM_CHUNK // KEY_CHUNK)]
                sweep(l, [own_job(f) for f in firsts] + [mate_job(f) for f in firsts])
                return 0
            lax.fori_loop(0, nch - 1, arrive, 0)
            relay_new()
            forward(l, nch - 1)
            chunk_wait(l, nch - 1)
            new_ready()
            tail = blocks((nch - 1) * COMM_CHUNK, plen)
            mate_tail(tail)
            sweep(l, [own_job(f) for f in tail] + [own_job(None)])

        @pl.when(l > 0)
        def _():
            forward(l, nch - 2)
            mid = nch // 2 * COMM_CHUNK
            for ch in range(nch // 2):
                chunk_wait(l, ch)
            early = (nch * 3 // 8) * COMM_CHUNK
            sweep(l, [own_job(f) for f in blocks(0, early)])
            for pair in range(grp // 2):
                q_copy(pair).wait_recv()
            sweep(l, [mate_job(f) for f in blocks(0, mid)])
            relay_new()
            forward(l, nch - 1)
            for ch in range(nch // 2, nch * 3 // 4):
                chunk_wait(l, ch)
            late = (nch * 3 // 4) * COMM_CHUNK
            sweep(l, [mate_job(f) for f in blocks(mid, late)])
            new_ready()
            for ch in range(nch * 3 // 4, nch):
                chunk_wait(l, ch)
            mate_tail(blocks(late, plen))
            sweep(l, [own_job(f) for f in blocks(early, plen)] + [own_job(None)])
        finish(0, att_own, 0, grp)
        kv_free(l)
        forward_next(l, 0)
        forward_next(l, 1)

        pltpu.make_async_copy(wo.at[l], wo_v, wo_sem).wait()
        y = mm(att_own[...], wo_v[pl.ds(pl.multiple_of(kvj * gcols, gcols), gcols), :])
        half = tok // 2
        for i, out in enumerate((k_out, v_out)):
            pieces = [nkv[lax.rem(l, 2), i, d * tok:d * tok + half, :] for d in range(n)]
            pieces += [nkv[lax.rem(l, 2), i, d * tok + half:(d + 1) * tok, :] for d in reversed(range(n))]
            tr[...] = jnp.concatenate(pieces, axis=0).astype(F32).T
            newc[l, i] = tr[my_rows, :].astype(BF16)
            pltpu.make_async_copy(newc.at[l, i], out.at[l], new_sem.at[i]).start()
        for i in range(2):
            o_copy(i).wait_recv()
        y = y + mm(att_rcv[...], wo_v[pl.ds(pl.multiple_of((1 - kvj) * gcols, gcols), gcols), :])
        x1 = (x_s[...].astype(F32) + y).astype(BF16)
        x_s[...] = x1
        h2[own_tok, :] = rms(x1, gains[1, l])
        h_copy = rcopy(h2.at[own_tok, :], h2.at[own_tok, :], h_sem.at[0], h_sem.at[1], sib)
        h_copy.start()

        for pair in range(grp // 2):
            q_copy(pair).wait_send()
        for i in range(2):
            o_copy(i).wait_send()
        for k in range(n // 2):
            nk_copy(k).wait_send()
        for k in range(1, n // 2):
            nk_relay(k).wait_send()
        h_copy.wait_recv()

        def gate_up(i):
            return mm(h2[...], gu[lax.rem(l * ngu + i, GU_SLOTS)])

        def activate(i, y):
            gate = y[:, :GU_CHUNK]
            act[:, pl.ds(gu_off(i), GU_CHUNK)] = (gate * jax.nn.sigmoid(gate) * y[:, GU_CHUNK:]).astype(BF16)

        def refill(i):
            @pl.when(l * ngu + i + GU_SLOTS < L * ngu)
            def _():
                gu_start(l * ngu + i + GU_SLOTS)

        for first in range(0, ngu, GU_UNROLL):
            steps = range(first, min(first + GU_UNROLL, ngu))
            for i in steps:
                gu_wait(l * ngu + i)
            ys = []
            for i in steps:
                ys.append(gate_up(i))
                if i + GU_SLOTS < ngu:
                    gu_start(l * ngu + i + GU_SLOTS)
            for i, y in zip(steps, ys):
                activate(i, y)
            for i in steps:
                if i + GU_SLOTS >= ngu:
                    refill(i)

        @pl.when(l + 1 < L)
        def _():
            wo_start(l + 1)
        for ch in range(2, 5):
            forward_next(l, ch)

        def p_copy(i):
            return rcopy(pr.at[i, sib_tok, :], part.at[i], p_send.at[i], p_recv.at[i], sib)

        def down(k, _):
            for i in (2 * k, 2 * k + 1):
                dn_copy(l * ndn + i).wait()
            for i in (2 * k, 2 * k + 1):
                slot = lax.rem(l * ndn + i, DN_SLOTS)
                pr[i] = mm(act[:, :ksplit], w2[slot, :ksplit, :]) + mm(act[:, ksplit:], w2[slot, ksplit:, :])
            for i in (2 * k, 2 * k + 1):
                p_copy(i).start()

                @pl.when(l * ndn + i + DN_SLOTS < L * ndn)
                def _():
                    dn_copy(l * ndn + i + DN_SLOTS).start()
            return 0
        lax.fori_loop(0, ndn // 2, down, 0)
        h_copy.wait_send()
        for ch in range(5, nch - 2):
            forward_next(l, ch)
        for i in range(ndn):
            cs = slice(i * DN_CHUNK, (i + 1) * DN_CHUNK)
            mine = x_s[:, cs].astype(F32) + pr[i, own_tok, :]
            p_copy(i).wait_recv()
            x_s[:, cs] = (mine + part[i]).astype(BF16)
            p_copy(i).wait_send()
        return 0

    lax.fori_loop(0, L, layer, 0)
    out_copy = pltpu.make_async_copy(x_s, x_out, in_sem.at[0])
    out_copy.start()
    for i, out in enumerate((k_out, v_out)):
        pltpu.make_async_copy(newc.at[:, i], out, new_sem.at[i]).wait()

    def drain(l, _):
        full = kv.at[lax.rem(l, 2), :, my_rows, :]
        rcopy(full, full, ss_sib.at[l], rs_sib.at[l], sib).wait_send()
        rcopy(full, full, ss_nbr.at[l], rs_nbr.at[l, 0], nbr).wait_send()
        return 0
    lax.fori_loop(0, L, drain, 0)
    out_copy.wait()


def solution(mesh):
    n = mesh.shape['cp']

    def device_fn(hidden, prefix_k, prefix_v, gain_attn, gain_mlp, w_query, w_key, w_value, w_out, w_gate, w_up, w_down):
        L, D, kvh, hd = w_key.shape
        heads = w_query.shape[2]
        tok = hidden.shape[0]
        plen = prefix_k.shape[1]
        cols = prefix_k.shape[2]
        ff = w_gate.shape[2]
        grp = heads // kvh
        half = tok // 2
        me = lax.axis_index('cp')
        pieces = jnp.stack([me, 2 * n - 1 - me])
        pos = (plen + pieces[:, None] * half + jnp.arange(half)).reshape(-1)
        inv_freq = ROPE_THETA ** (-jnp.arange(0, hd, 2, dtype=F32) / hd)
        ang = pos.astype(F32)[:, None] * inv_freq[None, :]
        cos_t = jnp.cos(ang)
        sin_t = jnp.sin(ang)
        pk = prefix_k.transpose(0, 2, 1)
        pv = prefix_v.transpose(0, 2, 1)
        wq = w_query.transpose(0, 2, 1, 3)
        wk = w_key.reshape(L, D * kvh, hd)
        wv = w_value.reshape(L, D * kvh, hd)
        wo = w_out.reshape(L, heads * hd, D)
        cfg = (n, L, D, heads, kvh, hd, tok, cols, plen)
        nch = plen // COMM_CHUNK
        rows = grp * tok
        dma = pltpu.SemaphoreType.DMA
        hbm = pl.BlockSpec(memory_space=pl.ANY)
        hid, nk, nv = pl.pallas_call(
            functools.partial(kernel, cfg),
            out_shape=(jax.ShapeDtypeStruct((tok, D), BF16),
                       jax.ShapeDtypeStruct((L, cols, n * tok), BF16),
                       jax.ShapeDtypeStruct((L, cols, n * tok), BF16)),
            in_specs=[hbm] * 14,
            out_specs=(hbm, hbm, hbm),
            scratch_shapes=[
                pltpu.VMEM((2, 2, hd, plen), BF16),
                pltpu.VMEM((GU_SLOTS, D, 2 * GU_CHUNK), BF16),
                pltpu.VMEM((DN_SLOTS, ff // 2, DN_CHUNK), BF16),
                pltpu.VMEM((D, heads * hd), BF16),
                pltpu.VMEM((D * kvh, 2 * hd), BF16),
                pltpu.VMEM((heads * hd, D), BF16),
                pltpu.VMEM((2, 2, n * tok, hd), BF16),
                pltpu.VMEM((kvh, 2, tok, hd), BF16),
                pltpu.VMEM((heads * tok, hd), BF16),
                pltpu.VMEM((rows, hd), BF16),
                pltpu.VMEM((2 * tok, D), BF16),
                pltpu.VMEM((2 * tok, ff // 2), BF16),
                pltpu.VMEM((D // DN_CHUNK, 2 * tok, DN_CHUNK), F32),
                pltpu.VMEM((D // DN_CHUNK, tok, DN_CHUNK), F32),
                pltpu.VMEM((tok, D), BF16),
                pltpu.VMEM((tok, grp * hd), BF16),
                pltpu.VMEM((tok, grp * hd), BF16),
                pltpu.VMEM((tok, grp * hd), BF16),
                pltpu.VMEM((2, rows, hd), F32),
                pltpu.VMEM((2, rows, hd), F32),
                pltpu.VMEM((2, rows, hd), F32),
                pltpu.VMEM((hd, n * tok), F32),
                pltpu.VMEM((2, L, 1, D), F32),
                pltpu.VMEM((2, L, D), BF16),
                pltpu.VMEM((2, tok, hd // 2), F32),
                pltpu.VMEM((hd, kvh * kvh * hd), BF16),
                pltpu.VMEM((L, 2, cols, n * tok), BF16),
                dma((L,)), dma((L,)), dma((L,)), dma((L,)),
                dma((L,)), dma((L, nch)), dma((L, nch)),
                dma((n // 2,)), dma((n // 2,)), dma((L, n)),
                dma((2, grp // 2)), dma((2, 2)), dma((2,)), dma((D // DN_CHUNK,)), dma((D // DN_CHUNK,)),
                dma, dma((2,)), dma, dma((GU_SLOTS, 2)), dma((DN_SLOTS,)), dma((5,)), dma((2,)), pltpu.SemaphoreType.REGULAR((2,)),
            ],
            compiler_params=pltpu.CompilerParams(collective_id=0, has_side_effects=True, vmem_limit_bytes=67043328),
            name='prefill',
        )(hidden, pk, pv, gain_attn, gain_mlp, wq, wk, wv, wo, w_gate, w_up, w_down, cos_t, sin_t)
        cache_k = jnp.concatenate([pk, nk], axis=2).transpose(0, 2, 1)
        cache_v = jnp.concatenate([pv, nv], axis=2).transpose(0, 2, 1)
        return hid, cache_k, cache_v

    in_specs = (P(('req', 'cp'), None), P(None, 'req', 'cp'), P(None, 'req', 'cp')) + (P(),) * 9
    out_specs = (P(('req', 'cp'), None), P(None, 'req', 'cp'), P(None, 'req', 'cp'))
    return jax.shard_map(device_fn, mesh=mesh, in_specs=in_specs, out_specs=out_specs, check_vma=False)
```

```python
import functools
import math

import jax
import jax.numpy as jnp
import numpy as np
from jax import lax
from jax.experimental import pallas as pl
from jax.experimental.pallas import tpu as pltpu
from jax.sharding import PartitionSpec as P

NORM_EPS = 1e-5
ROPE_THETA = 500000.0
MESH = pl.DeviceIdType.MESH
F32 = jnp.float32
BF16 = jnp.bfloat16

COMM_CHUNK = 1024
KEY_CHUNK = 512
LOOKAHEAD = 2
GU_CHUNK = 512
GU_UNROLL = 3
GU_SLOTS = 7
DN_CHUNK = 256
DN_SLOTS = 6


def rms(x, gain):
    xf = x.astype(F32)
    inv = lax.rsqrt(jnp.mean(xf * xf, axis=-1, keepdims=True) + NORM_EPS)
    return (xf * inv * gain.astype(F32)).astype(BF16)


def mm(a, b):
    return jnp.dot(a, b, preferred_element_type=F32)


def mm_t(a, b):
    return lax.dot_general(a, b, (((1,), (1,)), ((), ())), preferred_element_type=F32)


def kernel(cfg, x_in, pk, pv, g1, g2, wq, wk, wv, wo, wg, wu, wd, cos_ref, sin_ref,
           x_out, k_out, v_out,
           kv, gu, w2, wq_v, wkv_v, wo_v, nkv, kvs, qs, qr, h2, act, pr, part, x_s, att_own, att_snd, att_rcv,
           m_s, l_s, o_s, tr, gains, gain_v, trig, spread, newc,
           lsem, ss_sib, ss_nbr, ss_fwd, rs_sib, rs_nbr, rs_fwd, nk_s, nk_f, nk_r, q_sem, o_sem, h_sem, p_send, p_recv,
           wq_sem, wkv_sem, wo_sem, gu_sem, w2_sem, in_sem, new_sem, credit):
    n, L, D, heads, kvh, hd, tok, cols, plen = cfg
    grp = heads // kvh
    per = n // kvh
    grows = grp * tok
    gcols = grp * hd
    nch = plen // COMM_CHUNK
    ff_half = wg.shape[2] // 2
    ngu = pl.cdiv(ff_half, GU_CHUNK)
    ndn = D // DN_CHUNK
    ksplit = ff_half // 2 // 256 * 256 + 256
    scale = hd ** -0.5 * math.log2(math.e)

    me = lax.axis_index('cp')
    core = lax.rem(me, 2)
    chip = lax.div(me, 2)
    kvj = lax.div(me, per)
    quarter = lax.rem(me, per)
    sib = me + 1 - 2 * core
    nbr = kvj * per + lax.rem(quarter + 2, per)
    mate = 2 * (n // 2 - 1 - chip) + core

    def rows_of(dev):
        return pl.ds(pl.multiple_of(lax.rem(dev, per) * cols, cols), cols)

    my_rows = rows_of(me)
    nbr_rows = rows_of(nbr)
    sib_rows = rows_of(sib)
    sibnbr = kvj * per + lax.rem(lax.rem(sib, per) + 2, per)
    sibnbr_rows = rows_of(sibnbr)

    def rcopy(src, dst, s, r, dev):
        return pltpu.make_async_remote_copy(src_ref=src, dst_ref=dst, send_sem=s, recv_sem=r,
                                            device_id={'cp': dev}, device_id_type=MESH)

    def cpos(ch):
        return pl.ds(ch * COMM_CHUNK if isinstance(ch, int) else pl.multiple_of(ch * COMM_CHUNK, COMM_CHUNK), COMM_CHUNK)

    def wq_start(l):
        for h in range(heads):
            pltpu.make_async_copy(wq.at[l, h], wq_v.at[:, pl.ds(h * hd, hd)], wq_sem).start()
        for i, src in enumerate((wk, wv)):
            pltpu.make_async_copy(src.at[l], wkv_v.at[:, pl.ds(i * hd, hd)], wkv_sem.at[i]).start()

    def wo_start(l):
        pltpu.make_async_copy(wo.at[l], wo_v, wo_sem).start()

    def gu_off(i):
        return pl.multiple_of(jnp.minimum(i * GU_CHUNK, ff_half - GU_CHUNK), 128)

    def gu_copies(g):
        l = lax.div(g, ngu)
        off = pl.multiple_of(core * ff_half + gu_off(lax.rem(g, ngu)), 128)
        slot = lax.rem(g, GU_SLOTS)
        return (pltpu.make_async_copy(wg.at[l, :, pl.ds(off, GU_CHUNK)], gu.at[slot, :, pl.ds(0, GU_CHUNK)], gu_sem.at[slot, 0]),
                pltpu.make_async_copy(wu.at[l, :, pl.ds(off, GU_CHUNK)], gu.at[slot, :, pl.ds(GU_CHUNK, GU_CHUNK)], gu_sem.at[slot, 1]))

    def gu_start(g):
        for c in gu_copies(g):
            c.start()

    def gu_wait(g):
        for c in gu_copies(g):
            c.wait()

    def dn_copy(g):
        l = lax.div(g, ndn)
        row = pl.multiple_of(core * ff_half, 128)
        col = pl.multiple_of(lax.rem(g, ndn) * DN_CHUNK, DN_CHUNK)
        slot = lax.rem(g, DN_SLOTS)
        return pltpu.make_async_copy(wd.at[l, pl.ds(row, ff_half), pl.ds(col, DN_CHUNK)], w2.at[slot], w2_sem.at[slot])

    def own_local(l):
        b = lax.rem(l, 2)
        pltpu.make_async_copy(pk.at[l], kv.at[b, 0, my_rows, :], lsem.at[l]).start()
        pltpu.make_async_copy(pv.at[l], kv.at[b, 1, my_rows, :], lsem.at[l]).start()

    def own_send(l):
        b = lax.rem(l, 2)

        def body(ch, _):
            for i, src in enumerate((pk, pv)):
                rcopy(src.at[l, :, cpos(ch)], kv.at[b, i, my_rows, cpos(ch)], ss_nbr.at[l], rs_nbr.at[l, ch], nbr).start()
            return 0
        lax.fori_loop(0, nch, body, 0)
        for i, src in enumerate((pk, pv)):
            rcopy(src.at[l], kv.at[b, i, my_rows, :], ss_sib.at[l], rs_sib.at[l], sib).start()

    def forward(l, ch):
        blk = kv.at[lax.rem(l, 2), :, nbr_rows, cpos(ch)]
        rcopy(blk, blk, ss_nbr.at[l], rs_nbr.at[l, ch], nbr).wait_recv()
        rcopy(blk, blk, ss_fwd.at[l], rs_fwd.at[l, ch], sib).start()

    def chunk_wait(l, ch):
        blk = kv.at[lax.rem(l, 2), :, sibnbr_rows, cpos(ch)]
        rcopy(blk, blk, ss_fwd.at[l], rs_fwd.at[l, ch], sib).wait_recv()

    def forward_next(l, ch):
        @pl.when(l + 1 < L)
        def _():
            forward(l + 1, ch)

    def kv_free(l):
        full = kv.at[lax.rem(l, 2), :, nbr_rows, :]
        rcopy(full, full, ss_fwd.at[l], rs_fwd.at[l, 0], sib).wait_send()

        @pl.when(l + 2 < L)
        def _():
            pl.semaphore_signal(credit.at[0], inc=1, device_id={'cp': nbr}, device_id_type=MESH)
            pl.semaphore_signal(credit.at[1], inc=1, device_id={'cp': sib}, device_id_type=MESH)
            own_local(l + 2)

    barrier = pltpu.get_barrier_semaphore()
    for off in range(1, n):
        pl.semaphore_signal(barrier, inc=1, device_id={'cp': lax.rem(me + off, n)}, device_id_type=MESH)

    small = [pltpu.make_async_copy(src, dst, in_sem.at[i]) for i, (src, dst) in enumerate(
        [(x_in, x_s), (g1, gain_v.at[0]), (g2, gain_v.at[1])]
        + [(tab.at[pl.ds(pl.multiple_of(piece * (tok // 2), tok // 2), tok // 2), :], trig.at[t, pl.ds(p * (tok // 2), tok // 2), :])
           for t, tab in enumerate((cos_ref, sin_ref)) for p, piece in enumerate((me, 2 * n - 1 - me))])]
    for c in small:
        c.start()
    wq_start(0)
    pl.semaphore_wait(barrier, n - 1)
    own_send(0)
    own_local(0)
    wo_start(0)

    def prime_gu(g, _):
        gu_start(g)
        return 0
    lax.fori_loop(0, GU_SLOTS, prime_gu, 0)

    def prime_dn(g, _):
        dn_copy(g).start()
        return 0
    lax.fori_loop(0, DN_SLOTS, prime_dn, 0)

    own_local(1)

    src_row = lax.broadcasted_iota(jnp.int32, (hd, kvh * kvh * hd), 0)
    dst_col = lax.broadcasted_iota(jnp.int32, (hd, kvh * kvh * hd), 1)
    spread[...] = jnp.where(dst_col == src_row * kvh + lax.div(dst_col, kvh * hd) * (kvh * hd + 1), 1.0, 0.0).astype(BF16)
    for c in small:
        c.wait()
    for i in range(2):
        gain = gain_v[i].astype(F32)
        for l in range(L):
            gains[i, l] = gain[l:l + 1, :]

    def token_pos(t, dev):
        half = tok // 2
        return jnp.where(t < half, dev * half + t, (2 * n - 1 - dev) * half + t - half)

    def reset(st):
        m_s[st] = jnp.full((grows, hd), -jnp.inf, F32)
        l_s[st] = jnp.zeros((grows, hd), F32)
        o_s[st] = jnp.zeros((grows, hd), F32)

    def fold(st, at, s, pv_dot):
        width = s.shape[1]
        m_prev = m_s[st, at, :]
        m_new = jnp.maximum(m_prev, jnp.max(s, axis=1, keepdims=True))
        alpha = jnp.exp2((m_prev - m_new) * scale)
        p = jnp.exp2((s - jnp.concatenate([m_new] * (width // hd), axis=1)) * scale)
        lsum = p[:, :hd]
        for b in range(1, width // hd):
            lsum = lsum + p[:, b * hd:(b + 1) * hd]
        m_s[st, at, :] = m_new
        l_s[st, at, :] = alpha * l_s[st, at, :] + lsum
        o_s[st, at, :] = alpha * o_s[st, at, :] + pv_dot(p.astype(BF16))

    def sweep(l, jobs):
        b = lax.rem(l, 2)

        def keys(first):
            return pl.ds(first if isinstance(first, int) else pl.multiple_of(first, KEY_CHUNK), KEY_CHUNK)

        def score(job):
            _, at, q, first, dev = job
            if first is not None:
                return mm(q(), kv[b, 0, :, keys(first)])
            s = mm_t(q(), nkv[lax.rem(l, 2), 0])
            width = n * tok
            shape = (at.stop - at.start, width)
            tq = lax.broadcasted_iota(jnp.int32, shape, 0) & (tok - 1)
            col = lax.broadcasted_iota(jnp.int32, shape, 1)
            tk = col & (tok - 1)
            dk = col >> (tok.bit_length() - 1)
            return jnp.where(token_pos(tk, dk) <= token_pos(tq, dev), s, -jnp.inf)

        def mix(job):
            if job[3] is not None:
                return lambda p: mm_t(p, kv[b, 1, :, keys(job[3])])
            return lambda p: mm(p, nkv[lax.rem(l, 2), 1])

        ahead = [score(job) for job in jobs[:LOOKAHEAD]]
        for i, job in enumerate(jobs):
            fold(job[0], job[1], ahead.pop(0), mix(job))
            if i + LOOKAHEAD < len(jobs):
                ahead.append(score(jobs[i + LOOKAHEAD]))

    def finish(st, dst, first, last):
        o = (o_s[st, first * tok:last * tok, :] / jnp.sum(l_s[st, first * tok:last * tok, :], axis=1, keepdims=True)).astype(BF16)
        for h in range(first, last):
            dst[:, h * hd:(h + 1) * hd] = o[(h - first) * tok:(h - first + 1) * tok, :]

    own_q = pl.ds(pl.multiple_of(kvj * grows, grows), grows)
    own_tok = pl.ds(pl.multiple_of(core * tok, tok), tok)
    sib_tok = pl.ds(pl.multiple_of((1 - core) * tok, tok), tok)
    my_new = pl.ds(pl.multiple_of(me * tok, tok), tok)

    def layer(l, _):
        h = rms(x_s[...], gains[0, l])
        pltpu.make_async_copy(wo.at[l], wq_v, wq_sem).wait()
        cos_t = jnp.concatenate([trig[0], trig[0]], axis=1)
        sin_t = jnp.concatenate([-trig[1], trig[1]], axis=1)

        def rope(z):
            return (z * cos_t + pltpu.roll(z, hd // 2, 1) * sin_t).astype(BF16)

        def q_copy(pair):
            at = pl.ds(pl.multiple_of((1 - kvj) * grows + 2 * pair * tok, 2 * tok), 2 * tok)
            return rcopy(qs.at[at, :], qr.at[pl.ds(2 * pair * tok, 2 * tok), :], q_sem.at[0, pair], q_sem.at[1, pair], mate)

        def project_q(g, send):
            for pair in range(grp // 2):
                y = mm(h, wq_v[:, pl.ds(pl.multiple_of(g * gcols + 2 * pair * hd, hd), 2 * hd)])
                for s in range(2):
                    row = pl.multiple_of(g * grows + (2 * pair + s) * tok, tok)
                    qs[pl.ds(row, tok), :] = rope(y[:, s * hd:(s + 1) * hd])
                if send:
                    q_copy(pair).start()

        project_q(1 - kvj, True)
        project_q(kvj, False)
        hs = jnp.concatenate([h[:, b * hd:(b + 1) * hd] for b in range(D // hd)], axis=0)
        hs = mm(hs, spread[...]).astype(BF16)
        for b in range(D // hd):
            for j in range(kvh):
                act[j * tok:(j + 1) * tok, b * kvh * hd:(b + 1) * kvh * hd] = hs[b * tok:(b + 1) * tok, j * kvh * hd:(j + 1) * kvh * hd]
        for i, src in enumerate((wk, wv)):
            pltpu.make_async_copy(src.at[l], wkv_v.at[:, pl.ds(i * hd, hd)], wkv_sem.at[i]).wait()
        y = mm(act[:kvh * tok, :kvh * D], wkv_v[...])
        for j in range(kvh):
            kvs[j, 0] = rope(y[j * tok:(j + 1) * tok, :hd])
            kvs[j, 1] = y[j * tok:(j + 1) * tok, hd:].astype(BF16)

        @pl.when(l + 1 < L)
        def _():
            wq_start(l + 1)

        for i in range(2):
            nkv[lax.rem(l, 2), i, my_new, :] = kvs[kvj, i]

        def new_rows(src):
            return nkv.at[lax.rem(l, 2), :, pl.ds(pl.multiple_of(src * tok, tok), tok), :]

        def nk_copy(k):
            dst = lax.rem(me + 2 * k, n) if k else sib
            return rcopy(kvs.at[lax.div(dst, per)], nkv.at[lax.rem(l, 2), :, my_new, :], nk_s.at[k], nk_r.at[l, me], dst)

        def nk_relay(k):
            src = lax.rem(me + 2 * k, n)
            return rcopy(new_rows(src), new_rows(src), nk_f.at[k], nk_r.at[l, src], sib)

        def relay_new():
            for k in range(1, n // 2):
                src = lax.rem(me + 2 * k, n)
                rcopy(new_rows(src), new_rows(src), nk_s.at[k], nk_r.at[l, src], src).wait_recv()
                nk_relay(k).start()

        def new_ready():
            for k in range(n // 2):
                src = lax.rem(sib + 2 * k, n)
                rcopy(new_rows(src), new_rows(src), nk_s.at[k], nk_r.at[l, src], sib).wait_recv()

        for k in range(n // 2):
            nk_copy(k).start()

        @pl.when((l > 0) & (l + 1 < L))
        def _():
            pl.semaphore_wait(credit.at[0], 1)
            pl.semaphore_wait(credit.at[1], 1)

        @pl.when(l + 1 < L)
        def _():
            own_send(l + 1)

        full = kv.at[lax.rem(l, 2), :, my_rows, :]
        pltpu.make_async_copy(full, full, lsem.at[l]).wait()
        full = kv.at[lax.rem(l, 2), :, sib_rows, :]
        rcopy(full, full, ss_sib.at[l], rs_sib.at[l], sib).wait_recv()
        reset(0)
        reset(1)
        halves = (0, grp // 2, grp)

        def o_copy(i):
            at = pl.ds(halves[i] * hd, (halves[i + 1] - halves[i]) * hd)
            return rcopy(att_snd.at[:, at], att_rcv.at[:, at], o_sem.at[0, i], o_sem.at[1, i], mate)

        def own_job(first):
            return (0, slice(0, grows), lambda: qs[own_q, :], first, me)

        def mate_job(first, at=slice(0, grows)):
            return (1, at, lambda: qr[at, :], first, mate)

        def blocks(first, last):
            return [first + k * KEY_CHUNK for k in range((last - first) // KEY_CHUNK)]

        def mate_tail(firsts):
            for i in range(2):
                at = slice(halves[i] * tok, halves[i + 1] * tok)
                sweep(l, [mate_job(f, at) for f in firsts] + [mate_job(None, at)])
                finish(1, att_snd, halves[i], halves[i + 1])
                o_copy(i).start()

        @pl.when(l == 0)
        def _():
            for pair in range(grp // 2):
                q_copy(pair).wait_recv()

            def arrive(ch, _):
                forward(l, ch)
                chunk_wait(l, ch)
                first = ch * COMM_CHUNK
                firsts = [first + k * KEY_CHUNK for k in range(COMM_CHUNK // KEY_CHUNK)]
                sweep(l, [own_job(f) for f in firsts] + [mate_job(f) for f in firsts])
                return 0
            lax.fori_loop(0, nch - 1, arrive, 0)
            relay_new()
            forward(l, nch - 1)
            chunk_wait(l, nch - 1)
            new_ready()
            tail = blocks((nch - 1) * COMM_CHUNK, plen)
            mate_tail(tail)
            sweep(l, [own_job(f) for f in tail] + [own_job(None)])

        @pl.when(l > 0)
        def _():
            forward(l, nch - 2)
            mid = nch // 2 * COMM_CHUNK
            for ch in range(nch // 2):
                chunk_wait(l, ch)
            early = (nch * 3 // 8) * COMM_CHUNK
            sweep(l, [own_job(f) for f in blocks(0, early)])
            for pair in range(grp // 2):
                q_copy(pair).wait_recv()
            sweep(l, [mate_job(f) for f in blocks(0, mid)])
            relay_new()
            forward(l, nch - 1)
            for ch in range(nch // 2, nch * 3 // 4):
                chunk_wait(l, ch)
            late = (nch * 3 // 4) * COMM_CHUNK
            sweep(l, [mate_job(f) for f in blocks(mid, late)])
            new_ready()
            for ch in range(nch * 3 // 4, nch):
                chunk_wait(l, ch)
            mate_tail(blocks(late, plen))
            sweep(l, [own_job(f) for f in blocks(early, plen)] + [own_job(None)])
        finish(0, att_own, 0, grp)
        kv_free(l)
        forward_next(l, 0)
        forward_next(l, 1)

        pltpu.make_async_copy(wo.at[l], wo_v, wo_sem).wait()
        y = mm(att_own[...], wo_v[pl.ds(pl.multiple_of(kvj * gcols, gcols), gcols), :])
        half = tok // 2
        for i, out in enumerate((k_out, v_out)):
            pieces = [nkv[lax.rem(l, 2), i, d * tok:d * tok + half, :] for d in range(n)]
            pieces += [nkv[lax.rem(l, 2), i, d * tok + half:(d + 1) * tok, :] for d in reversed(range(n))]
            tr[...] = jnp.concatenate(pieces, axis=0).astype(F32).T
            newc[l, i] = tr[my_rows, :].astype(BF16)
            pltpu.make_async_copy(newc.at[l, i], out.at[l], new_sem.at[i]).start()
        for i in range(2):
            o_copy(i).wait_recv()
        y = y + mm(att_rcv[...], wo_v[pl.ds(pl.multiple_of((1 - kvj) * gcols, gcols), gcols), :])
        x1 = (x_s[...].astype(F32) + y).astype(BF16)
        x_s[...] = x1
        h2[own_tok, :] = rms(x1, gains[1, l])
        h_copy = rcopy(h2.at[own_tok, :], h2.at[own_tok, :], h_sem.at[0], h_sem.at[1], sib)
        h_copy.start()

        for pair in range(grp // 2):
            q_copy(pair).wait_send()
        for i in range(2):
            o_copy(i).wait_send()
        for k in range(n // 2):
            nk_copy(k).wait_send()
        for k in range(1, n // 2):
            nk_relay(k).wait_send()
        h_copy.wait_recv()

        def gate_up(i):
            return mm(h2[...], gu[lax.rem(l * ngu + i, GU_SLOTS)])

        def activate(i, y):
            gate = y[:, :GU_CHUNK]
            act[:, pl.ds(gu_off(i), GU_CHUNK)] = (gate * jax.nn.sigmoid(gate) * y[:, GU_CHUNK:]).astype(BF16)

        def refill(i):
            @pl.when(l * ngu + i + GU_SLOTS < L * ngu)
            def _():
                gu_start(l * ngu + i + GU_SLOTS)

        for first in range(0, ngu, GU_UNROLL):
            steps = range(first, min(first + GU_UNROLL, ngu))
            for i in steps:
                gu_wait(l * ngu + i)
            ys = []
            for i in steps:
                ys.append(gate_up(i))
                if i + GU_SLOTS < ngu:
                    gu_start(l * ngu + i + GU_SLOTS)
            for i, y in zip(steps, ys):
                activate(i, y)
            for i in steps:
                if i + GU_SLOTS >= ngu:
                    refill(i)

        @pl.when(l + 1 < L)
        def _():
            wo_start(l + 1)
        for ch in range(2, 5):
            forward_next(l, ch)

        def p_copy(i):
            return rcopy(pr.at[i, sib_tok, :], part.at[i], p_send.at[i], p_recv.at[i], sib)

        def down(k, _):
            for i in (2 * k, 2 * k + 1):
                dn_copy(l * ndn + i).wait()
            for i in (2 * k, 2 * k + 1):
                slot = lax.rem(l * ndn + i, DN_SLOTS)
                pr[i] = mm(act[:, :ksplit], w2[slot, :ksplit, :]) + mm(act[:, ksplit:], w2[slot, ksplit:, :])
            for i in (2 * k, 2 * k + 1):
                p_copy(i).start()

                @pl.when(l * ndn + i + DN_SLOTS < L * ndn)
                def _():
                    dn_copy(l * ndn + i + DN_SLOTS).start()
            return 0
        lax.fori_loop(0, ndn // 2, down, 0)
        h_copy.wait_send()
        for ch in range(5, nch - 2):
            forward_next(l, ch)
        for i in range(ndn):
            cs = slice(i * DN_CHUNK, (i + 1) * DN_CHUNK)
            mine = x_s[:, cs].astype(F32) + pr[i, own_tok, :]
            p_copy(i).wait_recv()
            x_s[:, cs] = (mine + part[i]).astype(BF16)
            p_copy(i).wait_send()
        return 0

    lax.fori_loop(0, L, layer, 0)
    out_copy = pltpu.make_async_copy(x_s, x_out, in_sem.at[0])
    out_copy.start()
    for i, out in enumerate((k_out, v_out)):
        pltpu.make_async_copy(newc.at[:, i], out, new_sem.at[i]).wait()

    def drain(l, _):
        full = kv.at[lax.rem(l, 2), :, my_rows, :]
        rcopy(full, full, ss_sib.at[l], rs_sib.at[l], sib).wait_send()
        rcopy(full, full, ss_nbr.at[l], rs_nbr.at[l, 0], nbr).wait_send()
        return 0
    lax.fori_loop(0, L, drain, 0)
    out_copy.wait()


def solution(mesh):
    n = mesh.shape['cp']

    def device_fn(hidden, prefix_k, prefix_v, gain_attn, gain_mlp, w_query, w_key, w_value, w_out, w_gate, w_up, w_down):
        L, D, kvh, hd = w_key.shape
        heads = w_query.shape[2]
        tok = hidden.shape[0]
        plen = prefix_k.shape[1]
        cols = prefix_k.shape[2]
        ff = w_gate.shape[2]
        grp = heads // kvh
        inv_freq = ROPE_THETA ** (-np.arange(0, hd, 2, dtype=np.float32) / np.float32(hd))
        ang = (plen + np.arange(n * tok)).astype(np.float32)[:, None] * inv_freq.astype(np.float32)[None, :]
        cos_t = np.cos(ang.astype(np.float64)).astype(np.float32)
        sin_t = np.sin(ang.astype(np.float64)).astype(np.float32)
        pk = prefix_k.transpose(0, 2, 1)
        pv = prefix_v.transpose(0, 2, 1)
        wq = w_query.transpose(0, 2, 1, 3)
        wk = w_key.reshape(L, D * kvh, hd)
        wv = w_value.reshape(L, D * kvh, hd)
        wo = w_out.reshape(L, heads * hd, D)
        cfg = (n, L, D, heads, kvh, hd, tok, cols, plen)
        nch = plen // COMM_CHUNK
        rows = grp * tok
        dma = pltpu.SemaphoreType.DMA
        hbm = pl.BlockSpec(memory_space=pl.ANY)
        hid, nk, nv = pl.pallas_call(
            functools.partial(kernel, cfg),
            out_shape=(jax.ShapeDtypeStruct((tok, D), BF16),
                       jax.ShapeDtypeStruct((L, cols, n * tok), BF16),
                       jax.ShapeDtypeStruct((L, cols, n * tok), BF16)),
            in_specs=[hbm] * 14,
            out_specs=(hbm, hbm, hbm),
            scratch_shapes=[
                pltpu.VMEM((2, 2, hd, plen), BF16),
                pltpu.VMEM((GU_SLOTS, D, 2 * GU_CHUNK), BF16),
                pltpu.VMEM((DN_SLOTS, ff // 2, DN_CHUNK), BF16),
                pltpu.VMEM((D, heads * hd), BF16),
                pltpu.VMEM((D * kvh, 2 * hd), BF16),
                pltpu.VMEM((heads * hd, D), BF16),
                pltpu.VMEM((2, 2, n * tok, hd), BF16),
                pltpu.VMEM((kvh, 2, tok, hd), BF16),
                pltpu.VMEM((heads * tok, hd), BF16),
                pltpu.VMEM((rows, hd), BF16),
                pltpu.VMEM((2 * tok, D), BF16),
                pltpu.VMEM((2 * tok, ff // 2), BF16),
                pltpu.VMEM((D // DN_CHUNK, 2 * tok, DN_CHUNK), F32),
                pltpu.VMEM((D // DN_CHUNK, tok, DN_CHUNK), F32),
                pltpu.VMEM((tok, D), BF16),
                pltpu.VMEM((tok, grp * hd), BF16),
                pltpu.VMEM((tok, grp * hd), BF16),
                pltpu.VMEM((tok, grp * hd), BF16),
                pltpu.VMEM((2, rows, hd), F32),
                pltpu.VMEM((2, rows, hd), F32),
                pltpu.VMEM((2, rows, hd), F32),
                pltpu.VMEM((hd, n * tok), F32),
                pltpu.VMEM((2, L, 1, D), F32),
                pltpu.VMEM((2, L, D), BF16),
                pltpu.VMEM((2, tok, hd // 2), F32),
                pltpu.VMEM((hd, kvh * kvh * hd), BF16),
                pltpu.VMEM((L, 2, cols, n * tok), BF16),
                dma((L,)), dma((L,)), dma((L,)), dma((L,)),
                dma((L,)), dma((L, nch)), dma((L, nch)),
                dma((n // 2,)), dma((n // 2,)), dma((L, n)),
                dma((2, grp // 2)), dma((2, 2)), dma((2,)), dma((D // DN_CHUNK,)), dma((D // DN_CHUNK,)),
                dma, dma((2,)), dma, dma((GU_SLOTS, 2)), dma((DN_SLOTS,)), dma((7,)), dma((2,)), pltpu.SemaphoreType.REGULAR((2,)),
            ],
            compiler_params=pltpu.CompilerParams(collective_id=0, has_side_effects=True, vmem_limit_bytes=67043328),
            name='prefill',
        )(hidden, pk, pv, gain_attn, gain_mlp, wq, wk, wv, wo, w_gate, w_up, w_down, jnp.asarray(cos_t), jnp.asarray(sin_t))
        cache_k = jnp.concatenate([pk, nk], axis=2).transpose(0, 2, 1)
        cache_v = jnp.concatenate([pv, nv], axis=2).transpose(0, 2, 1)
        return hid, cache_k, cache_v

    in_specs = (P(('req', 'cp'), None), P(None, 'req', 'cp'), P(None, 'req', 'cp')) + (P(),) * 9
    out_specs = (P(('req', 'cp'), None), P(None, 'req', 'cp'), P(None, 'req', 'cp'))
    return jax.shard_map(device_fn, mesh=mesh, in_specs=in_specs, out_specs=out_specs, check_vma=False)
```
